128 devices in a mesh: dp: 8 (over y, core), fsdp: 16 (over z, x).
Axes of the slice: x: 4, y: 4, z: 4, core: 2. Of those that a mesh axis runs over, the one named last changes fastest.
Arguments:
- grad_q: bfloat16 [8, 8192, 8192], P('dp', 'fsdp'), may hold values from -40 to 40, as said below
- grad_k: bfloat16 [8, 8192, 1024], P('dp', 'fsdp'), may hold values from -40 to 40
- grad_v: bfloat16 [8, 8192, 1024], P('dp', 'fsdp'), may hold values from -40 to 40
- proj_q: bfloat16 [8192, 512], P('fsdp'), may hold values from -5 to 5, as said below
- proj_k: bfloat16 [8192, 512], P('fsdp'), may hold values from -5 to 5
- proj_v: bfloat16 [8192, 512], P('fsdp'), may hold values from -5 to 5
- weight_q: bfloat16 [8192, 8192], P('fsdp', 'dp'), may hold values from -4 to 4
- key_weight_matrix: bfloat16 [8192, 1024], P('fsdp', 'dp'), may hold values from -4 to 4
- value_weight_matrix: bfloat16 [8192, 1024], P('fsdp', 'dp'), may hold values from -4 to 4
- comp_q: bfloat16 [8192, 8192], P('fsdp', 'dp'), may hold values from -0.0039978027 to 0.0039978027
- key_compensation: bfloat16 [8192, 1024], P('fsdp', 'dp'), may hold values from -0.0039978027 to 0.0039978027
- value_compensation: bfloat16 [8192, 1024], P('fsdp', 'dp'), may hold values from -0.0039978027 to 0.0039978027
- avg_q: float32 [512, 8192], P('fsdp', 'dp'), may hold values from -1.5 to 1.5
- key_first_moment: float32 [512, 1024], P('fsdp', 'dp'), may hold values from -1.5 to 1.5
- value_first_moment: float32 [512, 1024], P('fsdp', 'dp'), may hold values from -1.5 to 1.5
- sq_q: float32 [512, 8192], P('fsdp', 'dp'), may hold values from 0.001 to 0.1
- key_second_moment: float32 [512, 1024], P('fsdp', 'dp'), may hold values from 0.001 to 0.1
- value_second_moment: float32 [512, 1024], P('fsdp', 'dp'), may hold values from 0.001 to 0.1
Outputs:
- new_weight_q: float32 [8192, 8192], P('fsdp', 'dp')
- new_weight_k: float32 [8192, 1024], P('fsdp', 'dp')
- new_weight_v: float32 [8192, 1024], P('fsdp', 'dp')
- new_avg_q: float32 [512, 8192], P('fsdp', 'dp')
- new_avg_k: float32 [512, 1024], P('fsdp', 'dp')
- new_avg_v: float32 [512, 1024], P('fsdp', 'dp')
- new_sq_q: float32 [512, 8192], P('fsdp', 'dp')
- new_sq_k: float32 [512, 1024], P('fsdp', 'dp')
- new_sq_v: float32 [512, 1024], P('fsdp', 'dp')
The draws below stay inside these ranges and needn't reach their ends.
Inputs may be any that keep to these rules, and one draw needn't show every extreme that they name: `grad_q`: each partial of the gradients is real-valued and of full rank. `proj_q`: projectors are real-valued and of full rank 512.
All inputs are finite; a program needn't handle non-finite values.
Results may differ from the reference program's by a relative error of at most 0.00044.
Values may be sent and summed in bfloat16 or wider, within the bound.
No kernel may reach another device: no remote copies, remote signals or barrier semaphores. Data moves between devices by JAX's collectives and lax.ppermute only.
A program may use at most 128 MiB of HBM per device.

```python
import math
import jax
import jax.numpy as jnp
from jax import lax

MODEL_WIDTH = 8192
QUERY_OUTPUTS = 8192
KEY_VALUE_OUTS = 1024
PROJECT_RANK = 512
STEP = 10
N_DP = 8
N_FSDP = 16


def column_scales(columns):
    steps_along = jnp.arange(columns, dtype=jnp.float32) / max(columns - 1, 1)
    return jnp.exp(math.log(10.0) * steps_along)


def row_profile(key, matrix_tag):
    return jax.random.uniform(jax.random.fold_in(key, 100 + matrix_tag), (MODEL_WIDTH,), jnp.float32, 0.5, 1.0)


def gradient_sampler(key, matrix_tag, columns):
    own_key = jax.random.fold_in(key, matrix_tag)
    scales = column_scales(columns)
    row_weights = row_profile(key, matrix_tag)
    column_mix = jax.random.uniform(jax.random.fold_in(own_key, 14), (columns,), jnp.float32, -1.5, 1.5)
    coherent = 0.1 * row_weights[:, None] * column_mix[None, :]
    level_grid = jnp.exp(jax.random.uniform(jax.random.fold_in(own_key, 15), (N_FSDP, N_DP), jnp.float32, -1.5, 0.0))
    levels = jnp.repeat(jnp.repeat(level_grid, MODEL_WIDTH // N_FSDP, axis=0), columns // N_DP, axis=1)
    random_part = jax.random.truncated_normal(jax.random.fold_in(own_key, 13), -3.5, 3.5, (N_DP, MODEL_WIDTH, columns), jnp.float32)
    values = (random_part + coherent[None]) * levels[None] * scales
    return values.astype(jnp.bfloat16)


def projector_draw(key, matrix_tag):
    own_key = jax.random.fold_in(key, 10 + matrix_tag)
    scales = column_scales(PROJECT_RANK) / math.sqrt(MODEL_WIDTH)
    row_weights = row_profile(key, matrix_tag)
    rank_mix = jax.random.uniform(jax.random.fold_in(own_key, 23), (PROJECT_RANK,), jnp.float32, -1.7, 1.7)
    coherent = 0.1 * row_weights[:, None] * rank_mix[None, :]
    random_part = jax.random.truncated_normal(jax.random.fold_in(own_key, 22), -3.8, 3.8, (MODEL_WIDTH, PROJECT_RANK), jnp.float32)
    values = (random_part + coherent) * scales
    return values.astype(jnp.bfloat16)


def draw_grad_q(key, part):
    return gradient_sampler(key, 1, QUERY_OUTPUTS)


def draw_grad_k(key, part):
    return gradient_sampler(key, 2, KEY_VALUE_OUTS)


def draw_grad_v(key, part):
    return gradient_sampler(key, 3, KEY_VALUE_OUTS)


def draw_proj_q(key, part):
    return projector_draw(key, 1)


def draw_proj_k(key, part):
    return projector_draw(key, 2)


def draw_proj_v(key, part):
    return projector_draw(key, 3)


def block_levels(stream_key, shape, shards, least, high):
    factor_of, own = 1.0, jax.random.fold_in(stream_key, 6)
    for axis_at, parts in shards:
        draws = jnp.exp(jax.random.uniform(jax.random.fold_in(own, axis_at), (parts,), jnp.float32, least / len(shards), high / len(shards)))
        factor_of = factor_of * jnp.repeat(draws, shape[axis_at] // parts).reshape([-1 if axis == axis_at else 1 for axis in range(len(shape))])
    return factor_of


def normal_values(rng, extent, scale, bound, cuts=(), kind=jnp.bfloat16):
    factor_of = block_levels(rng, extent, cuts, -0.22, 0.18) if cuts else 1.0
    entries = jax.random.normal(rng, extent, jnp.float32) * scale * factor_of
    return jnp.minimum(jnp.maximum(entries, -bound), bound).astype(kind)


def setup_inputs(seed: int = 0) -> dict:
    key_list = jax.random.split(jax.random.key(seed), 19)
    return {
        "grad_q": draw_grad_q(jax.random.fold_in(key_list[18], 71), 0),
        "grad_k": draw_grad_k(jax.random.fold_in(key_list[18], 71), 0),
        "grad_v": draw_grad_v(jax.random.fold_in(key_list[18], 71), 0),
        "proj_q": draw_proj_q(jax.random.fold_in(key_list[18], 71), 0),
        "proj_k": draw_proj_k(jax.random.fold_in(key_list[18], 71), 0),
        "proj_v": draw_proj_v(jax.random.fold_in(key_list[18], 71), 0),
        "weight_q": normal_values(key_list[6], (MODEL_WIDTH, QUERY_OUTPUTS), 0.25, 4.0, ((0, 16), (1, 8))),
        "key_weight_matrix": normal_values(key_list[7], (MODEL_WIDTH, KEY_VALUE_OUTS), 0.25, 4.0, ((0, 16), (1, 8))),
        "value_weight_matrix": normal_values(key_list[8], (MODEL_WIDTH, KEY_VALUE_OUTS), 0.25, 4.0, ((0, 16), (1, 8))),
        "comp_q": jnp.clip(jax.random.uniform(key_list[9], (MODEL_WIDTH, QUERY_OUTPUTS), jnp.float32, -0.0039978027, 0.0039978027) * block_levels(key_list[9], (MODEL_WIDTH, QUERY_OUTPUTS), ((0, 16), (1, 8)), -0.4, 0.0), -0.0039978027, 0.0039978027).astype(jnp.bfloat16),
        "key_compensation": jnp.clip(jax.random.uniform(key_list[10], (MODEL_WIDTH, KEY_VALUE_OUTS), jnp.float32, -0.0039978027, 0.0039978027) * block_levels(key_list[10], (MODEL_WIDTH, KEY_VALUE_OUTS), ((0, 16), (1, 8)), -0.4, 0.0), -0.0039978027, 0.0039978027).astype(jnp.bfloat16),
        "value_compensation": jnp.clip(jax.random.uniform(key_list[11], (MODEL_WIDTH, KEY_VALUE_OUTS), jnp.float32, -0.0039978027, 0.0039978027) * block_levels(key_list[11], (MODEL_WIDTH, KEY_VALUE_OUTS), ((0, 16), (1, 8)), -0.4, 0.0), -0.0039978027, 0.0039978027).astype(jnp.bfloat16),
        "avg_q": normal_values(key_list[12], (PROJECT_RANK, QUERY_OUTPUTS), 0.1, 1.5, ((0, 16), (1, 8)), jnp.float32),
        "key_first_moment": normal_values(key_list[13], (PROJECT_RANK, KEY_VALUE_OUTS), 0.1, 1.5, ((0, 16), (1, 8)), jnp.float32),
        "value_first_moment": normal_values(key_list[14], (PROJECT_RANK, KEY_VALUE_OUTS), 0.1, 1.5, ((0, 16), (1, 8)), jnp.float32),
        "sq_q": jnp.clip(jnp.exp(math.log(0.1) - 4.6051702 * jax.random.uniform(key_list[15], (PROJECT_RANK, QUERY_OUTPUTS), jnp.float32) ** block_levels(key_list[15], (PROJECT_RANK, QUERY_OUTPUTS), ((0, 16), (1, 8)), -0.2, 0.2)), 0.001, 0.1),
        "key_second_moment": jnp.clip(jnp.exp(math.log(0.1) - 4.6051702 * jax.random.uniform(key_list[16], (PROJECT_RANK, KEY_VALUE_OUTS), jnp.float32) ** block_levels(key_list[16], (PROJECT_RANK, KEY_VALUE_OUTS), ((0, 16), (1, 8)), -0.2, 0.2)), 0.001, 0.1),
        "value_second_moment": jnp.clip(jnp.exp(math.log(0.1) - 4.6051702 * jax.random.uniform(key_list[17], (PROJECT_RANK, KEY_VALUE_OUTS), jnp.float32) ** block_levels(key_list[17], (PROJECT_RANK, KEY_VALUE_OUTS), ((0, 16), (1, 8)), -0.2, 0.2)), 0.001, 0.1),
    }


def project_sum(gradient, projector):

    def accumulate(carry, slab):
        product = lax.dot_general(projector, slab, (((0,), (0,)), ((), ())), preferred_element_type=jnp.float32)
        return (carry + product, None)
    start_sum = jnp.zeros((projector.shape[1], gradient.shape[2]), jnp.float32)
    return lax.scan(accumulate, start_sum, gradient)[0]

def adam_apply(projected, clip_factor, first_moment, second_moment):
    scaled = clip_factor * projected
    new_avg = 0.9 * first_moment + 0.1 * scaled
    new_sq = 0.95 * second_moment + 0.05 * scaled * scaled
    correct_one = 1.0 - 0.9 ** STEP
    correct_two = 1.0 - 0.95 ** STEP
    update = new_avg / correct_one / (jnp.sqrt(new_sq / correct_two) + 1e-08)
    return (new_avg, new_sq, update.astype(jnp.bfloat16))

def kahan_apply(weight, compensation, projector, update):
    delta = -0.04 * jnp.dot(projector, update, preferred_element_type=jnp.float32)
    return weight.astype(jnp.float32) + (delta + compensation.astype(jnp.float32))

def reference(grad_q, grad_k, grad_v, proj_q, proj_k, proj_v, weight_q, key_weight_matrix, value_weight_matrix, comp_q, key_compensation, value_compensation, avg_q, key_first_moment, value_first_moment, sq_q, key_second_moment, value_second_moment):
    gradients = (grad_q, grad_k, grad_v)
    projectors = (proj_q, proj_k, proj_v)
    weights = (weight_q, key_weight_matrix, value_weight_matrix)
    comps = (comp_q, key_compensation, value_compensation)
    avgs = (avg_q, key_first_moment, value_first_moment)
    squares = (sq_q, key_second_moment, value_second_moment)
    projected = [project_sum(gradient, projector) for gradient, projector in zip(gradients, projectors)]
    square_sum = jnp.zeros((), jnp.float32)
    for member in projected:
        square_sum = square_sum + jnp.sum(member * member)
    clipping_threshold = math.sqrt(PROJECT_RANK * (QUERY_OUTPUTS + 2 * KEY_VALUE_OUTS))
    clip_factor = jnp.minimum(1.0, clipping_threshold / jnp.sqrt(square_sum + 1e-06))
    new_weights, new_avgs, new_sqs = ([], [], [])
    for index_mat in range(3):
        new_avg, new_sq, update = adam_apply(projected[index_mat], clip_factor, avgs[index_mat], squares[index_mat])
        new_weights.append(kahan_apply(weights[index_mat], comps[index_mat], projectors[index_mat], update))
        new_avgs.append(new_avg)
        new_sqs.append(new_sq)
    return (new_weights[0], new_weights[1], new_weights[2], new_avgs[0], new_avgs[1], new_avgs[2], new_sqs[0], new_sqs[1], new_sqs[2])
```

```python
import math

import jax
import jax.numpy as jnp
from jax import lax
from jax.experimental import pallas as pl
from jax.experimental.pallas import tpu as pltpu
from jax.sharding import Mesh
from jax.sharding import PartitionSpec as P

QUERY_OUTPUTS = 8192
KEY_VALUE_OUTS = 1024
PROJECT_RANK = 512
STEP = 10
DP = ("dp_0", "dp_1")
FSDP = ("fsdp_0", "fsdp_1")
ALL = ("dp_0", "dp_1", "fsdp_0", "fsdp_1")

ROWS = 512
RANK_ROWS = 32
BLOCK = 128
WQ, WK = 1024, 128
WIDTH = WQ + 2 * WK
SCALE_ROWS = 16


F32 = jnp.float32
BF16 = jnp.bfloat16
F16 = jnp.float16


def pairs(move):
    found = []
    for y in range(4):
        for c in range(2):
            for z in range(4):
                for x in range(4):
                    ty, tc, tz, tx = move(y, c, z, x)
                    source = ((y * 2 + c) * 4 + z) * 4 + x
                    found.append((source, ((ty * 2 + tc) * 4 + tz) * 4 + tx))
    return found


def along_first(d):
    return pairs(lambda y, c, z, x: (y, c, (z + d) % 4, x) if c == 0 else (y, c, z, (x + d) % 4))


def along_second(d):
    return pairs(lambda y, c, z, x: (y, c, z, (x + d) % 4) if c == 0 else (y, c, (z + d) % 4, x))


def along_y(d):
    return pairs(lambda y, c, z, x: ((y + d) % 4, c, z, x))


CORE_SWAP = pairs(lambda y, c, z, x: (y, 1 - c, z, x))
BUTTERFLY = (
    CORE_SWAP,
    pairs(lambda y, c, z, x: (y ^ 1, c, z, x)),
    pairs(lambda y, c, z, x: (3 - y, c, z, x)),
    pairs(lambda y, c, z, x: (y, c, z ^ 1, x)),
    pairs(lambda y, c, z, x: (y, c, 3 - z, x)),
    pairs(lambda y, c, z, x: (y, c, z, x ^ 1)),
    pairs(lambda y, c, z, x: (y, c, z, 3 - x)),
)


def send(value, route):
    return lax.ppermute(value, ALL, route)


def take_columns(where, grads):
    def body(where_ref, q_ref, k_ref, v_ref, out_ref):
        out_ref[:, :WQ] = q_ref[...]
        out_ref[:, WQ : WQ + WK] = k_ref[...]
        out_ref[:, WQ + WK :] = v_ref[...]

    def column(i, where):
        return (0, 2 * i + 1 - where[0])

    return pl.pallas_call(
        body,
        grid_spec=pltpu.PrefetchScalarGridSpec(
            num_scalar_prefetch=1,
            grid=(4,),
            in_specs=[
                pl.BlockSpec((ROWS, WQ), column),
                pl.BlockSpec((ROWS, WK), column),
                pl.BlockSpec((ROWS, WK), column),
            ],
            out_specs=pl.BlockSpec((ROWS, WIDTH), lambda i, where: (0, i)),
        ),
        out_shape=jax.ShapeDtypeStruct((ROWS, 4 * WIDTH), BF16),
        name="take_columns",
    )(where, *grads)


def project(where, grads, received, projectors, offsets, scaled):
    count = len(offsets)

    def body(where_ref, q_ref, k_ref, v_ref, other_ref, pq_ref, pk_ref, pv_ref, *rest):
        outs, transposed = rest[:count], rest[count]

        @pl.when(pl.program_id(0) == 0)
        def _():
            core = where_ref[0]
            at = lax.broadcasted_iota(jnp.int32, (BLOCK, PROJECT_RANK), 0)
            rank = lax.broadcasted_iota(jnp.int32, (BLOCK, PROJECT_RANK), 1)
            outer, inner = at // RANK_ROWS, at % RANK_ROWS
            for n, d in enumerate(offsets):
                a = (where_ref[1] + d) % 4
                straight = a * BLOCK + at
                crossed = outer * BLOCK + a * RANK_ROWS + inner
                wanted = jnp.where(core == 0, straight, crossed)
                pick = jnp.where(rank == wanted, 1.0, 0.0).astype(BF16)
                for m, p_ref in enumerate((pq_ref, pk_ref, pv_ref)):
                    rows = lax.dot_general(
                        pick, p_ref[...], (((1,), (1,)), ((), ())), preferred_element_type=F32
                    )
                    transposed[n, m] = rows.astype(BF16)

        cuts = ((0, WQ), (WQ, WQ + WK), (WQ + WK, WIDTH))
        for n in range(count):
            for m, own_ref in enumerate((q_ref, k_ref, v_ref)):
                lo, hi = cuts[m]
                left = transposed[n, m]
                product = jnp.dot(left, own_ref[...], preferred_element_type=F32)
                product += jnp.dot(left, other_ref[:, lo:hi], preferred_element_type=F32)
                if scaled[n]:
                    largest = jnp.max(jnp.abs(product), axis=0, keepdims=True)
                    scale = jnp.clip(8192.0 / jnp.maximum(largest, 1e-30), 0.03125, 32768.0)
                    scale = scale.astype(BF16).astype(F32)
                    outs[n][:BLOCK, lo:hi] = product * scale
                    outs[n][BLOCK:, lo:hi] = jnp.broadcast_to(scale, (SCALE_ROWS, hi - lo))
                else:
                    outs[n][:, lo:hi] = product

    def column(i, where):
        return (0, 2 * i + where[0])

    heights = [BLOCK + SCALE_ROWS if s else BLOCK for s in scaled]
    return pl.pallas_call(
        body,
        grid_spec=pltpu.PrefetchScalarGridSpec(
            num_scalar_prefetch=1,
            grid=(4,),
            in_specs=[
                pl.BlockSpec((ROWS, WQ), column),
                pl.BlockSpec((ROWS, WK), column),
                pl.BlockSpec((ROWS, WK), column),
                pl.BlockSpec((ROWS, WIDTH), lambda i, where: (0, i)),
                *[pl.BlockSpec((ROWS, PROJECT_RANK), lambda i, where: (0, 0))] * 3,
            ],
            out_specs=[pl.BlockSpec((h, WIDTH), lambda i, where: (0, i)) for h in heights],
            scratch_shapes=[pltpu.VMEM((count, 3, BLOCK, ROWS), BF16)],
        ),
        out_shape=[jax.ShapeDtypeStruct((h, 4 * WIDTH), F32) for h in heights],
        name="project",
    )(where, *grads, received, *projectors)


def finish_sum(pieces):
    def body(a_ref, b_ref, c_ref, d_ref, sum_ref, square_ref):
        total = (a_ref[...] + b_ref[...]) + (c_ref[...] + d_ref[...])
        sum_ref[...] = total
        square_ref[...] = jnp.broadcast_to(jnp.sum(total * total, keepdims=True), (8, 128))

    return pl.pallas_call(
        body,
        out_shape=[
            jax.ShapeDtypeStruct((RANK_ROWS, WIDTH), F32),
            jax.ShapeDtypeStruct((8, 128), F32),
        ],
        name="finish_sum",
    )(*pieces)


def adam(projected, square_sum, avgs, squares):
    threshold = math.sqrt(PROJECT_RANK * (QUERY_OUTPUTS + 2 * KEY_VALUE_OUTS))
    correct_one = 1.0 - 0.9**STEP
    correct_two = 1.0 - 0.95**STEP

    def body(p_ref, s_ref, *rest):
        avg_refs, sq_refs = rest[:3], rest[3:6]
        new_avg_refs, new_sq_refs, update_ref = rest[6:9], rest[9:12], rest[12]
        clip = jnp.minimum(1.0, threshold / jnp.sqrt(s_ref[0:1, 0:1] + 1e-06))
        at = 0
        for m in range(3):
            wide = avg_refs[m].shape[1]
            scaled = clip * p_ref[:, at : at + wide]
            new_avg = 0.9 * avg_refs[m][...] + 0.1 * scaled
            new_sq = 0.95 * sq_refs[m][...] + 0.05 * scaled * scaled
            new_avg_refs[m][...] = new_avg
            new_sq_refs[m][...] = new_sq
            update = new_avg / correct_one / (jnp.sqrt(new_sq / correct_two) + 1e-08)
            update_ref[:, at : at + wide] = update.astype(BF16)
            at += wide

    like = [jax.ShapeDtypeStruct(a.shape, F32) for a in avgs]
    return pl.pallas_call(
        body,
        out_shape=[*like, *like, jax.ShapeDtypeStruct((RANK_ROWS, WIDTH), BF16)],
        name="adam",
    )(projected, square_sum, *avgs, *squares)


def apply_updates(where, gathered, projectors, weights, comps):
    tile = 128

    def body(where_ref, *refs):
        parts, (pq, pk, pv), ws, cs = refs[:4], refs[4:7], refs[7:10], refs[10:13]
        outs, update = refs[13:16], refs[16]

        @pl.when(pl.program_id(0) == 0)
        def _():
            core, first, second = where_ref[0], where_ref[1], where_ref[2]
            for d in range(4):
                for k in range(4):
                    far = (first + 4 - d) % 4
                    near = (second + 4 - k) % 4
                    z = jnp.where(core == 0, far, near)
                    x = jnp.where(core == 0, near, far)
                    at = pl.multiple_of(z * BLOCK + x * RANK_ROWS, RANK_ROWS)
                    update[pl.ds(at, RANK_ROWS), :] = parts[d][k * RANK_ROWS : (k + 1) * RANK_ROWS, :]

        at = 0
        for m, p_ref in enumerate((pq, pk, pv)):
            wide = ws[m].shape[1]
            product = jnp.dot(p_ref[...], update[:, at : at + wide], preferred_element_type=F32)
            outs[m][...] = ws[m][...].astype(F32) + (-0.04 * product + cs[m][...].astype(F32))
            at += wide

    def rows(i, where):
        return (i, 0)

    tall = [pl.BlockSpec((tile, w.shape[1]), rows) for w in weights]
    return pl.pallas_call(
        body,
        grid_spec=pltpu.PrefetchScalarGridSpec(
            num_scalar_prefetch=1,
            grid=(ROWS // tile,),
            in_specs=[
                *[pl.BlockSpec((BLOCK, WIDTH), lambda i, where: (0, 0))] * 4,
                *[pl.BlockSpec((tile, PROJECT_RANK), rows)] * 3,
                *tall,
                *tall,
            ],
            out_specs=tall,
            scratch_shapes=[pltpu.VMEM((PROJECT_RANK, WIDTH), BF16)],
        ),
        out_shape=[jax.ShapeDtypeStruct(w.shape, F32) for w in weights],
        name="apply_updates",
    )(where, *gathered, *projectors, *weights, *comps)


def shards(
    grad_q,
    grad_k,
    grad_v,
    proj_q,
    proj_k,
    proj_v,
    weight_q,
    key_weight_matrix,
    value_weight_matrix,
    comp_q,
    key_compensation,
    value_compensation,
    avg_q,
    key_first_moment,
    value_first_moment,
    sq_q,
    key_second_moment,
    value_second_moment,
):
    grads = (grad_q[0], grad_k[0], grad_v[0])
    projectors = (proj_q, proj_k, proj_v)
    y, core, z, x = (lax.axis_index(name) for name in ALL)
    first = jnp.where(core == 0, z, x)
    second = jnp.where(core == 0, x, z)
    where = jnp.stack([core, first, second]).astype(jnp.int32)

    received = send(take_columns(where, grads), CORE_SWAP)

    near = project(where, grads, received, projectors, (1, 3), (True, True))
    far = project(where, grads, received, projectors, (2, 0), (True, False))
    arrived = [send(part.astype(F16), along_first(d)) for d, part in ((1, near[0]), (3, near[1]), (2, far[0]))]

    def rank_rows(b):
        at = b * RANK_ROWS
        total = lax.dynamic_slice_in_dim(far[1], at, RANK_ROWS, axis=0)
        for part in arrived:
            scale = part[BLOCK : BLOCK + 1].astype(F32)
            total = total + lax.dynamic_slice_in_dim(part, at, RANK_ROWS, axis=0).astype(F32) / scale
        return total

    parts = {d: rank_rows((second + d) % 4) for d in (1, 3, 2, 0)}
    arrived_two = [send(parts[d], along_second(d)) for d in (1, 3, 2)]

    def columns(b):
        at = b * WIDTH
        total = lax.dynamic_slice_in_dim(parts[0], at, WIDTH, axis=1)
        for part in arrived_two:
            total = total + lax.dynamic_slice_in_dim(part, at, WIDTH, axis=1)
        return total

    blocks = {d: columns((y + d) % 4) for d in (1, 3, 2, 0)}
    arrived_three = [send(blocks[d], along_y(d)) for d in (1, 3, 2)]
    projected, square_sum = finish_sum((blocks[0], *arrived_three))
    for route in BUTTERFLY:
        square_sum = square_sum + send(square_sum, route)

    *moments, update = adam(
        projected,
        square_sum,
        (avg_q, key_first_moment, value_first_moment),
        (sq_q, key_second_moment, value_second_moment),
    )

    held = jnp.concatenate([update, *[send(update, along_second(d)) for d in (1, 2, 3)]], axis=0)
    gathered = [held, *[send(held, along_first(d)) for d in (1, 2, 3)]]
    new_weights = apply_updates(
        where,
        gathered,
        projectors,
        (weight_q, key_weight_matrix, value_weight_matrix),
        (comp_q, key_compensation, value_compensation),
    )
    return (*new_weights, *moments)


def solution(mesh):
    split = Mesh(mesh.devices.reshape(4, 2, 4, 4), ALL)
    return jax.shard_map(
        shards,
        mesh=split,
        in_specs=(*[P(DP, FSDP, None)] * 3, *[P(FSDP, None)] * 3, *[P(FSDP, DP)] * 12),
        out_specs=(*[P(FSDP, DP)] * 9,),
        check_vma=False,
    )
```

```python
import math

import jax
import jax.numpy as jnp
from jax import lax
from jax.experimental import pallas as pl
from jax.experimental.pallas import tpu as pltpu
from jax.sharding import Mesh
from jax.sharding import PartitionSpec as P

QUERY_OUTPUTS = 8192
KEY_VALUE_OUTS = 1024
PROJECT_RANK = 512
STEP = 10
DP = ("dp_0", "dp_1")
FSDP = ("fsdp_0", "fsdp_1")
ALL = ("dp_0", "dp_1", "fsdp_0", "fsdp_1")

ROWS = 512
RANK_ROWS = 32
BLOCK = 128
WQ, WK = 1024, 128
WIDTH = WQ + 2 * WK
HALF = WIDTH // 2
ORDER = (1, 3, 2, 0)
SEGMENTS = (((0, 0, HALF, 0),), ((0, HALF, WQ - HALF, 0), (1, 0, WK, WQ - HALF), (2, 0, WK, WQ - HALF + WK)))


F32 = jnp.float32
BF16 = jnp.bfloat16
F16 = jnp.float16


def pairs(move):
    found = []
    for y in range(4):
        for c in range(2):
            for z in range(4):
                for x in range(4):
                    ty, tc, tz, tx = move(y, c, z, x)
                    source = ((y * 2 + c) * 4 + z) * 4 + x
                    found.append((source, ((ty * 2 + tc) * 4 + tz) * 4 + tx))
    return found


def along_first(d):
    return pairs(lambda y, c, z, x: (y, c, (z + d) % 4, x) if c == 0 else (y, c, z, (x + d) % 4))


def along_second(d):
    return pairs(lambda y, c, z, x: (y, c, z, (x + d) % 4) if c == 0 else (y, c, (z + d) % 4, x))


def along_y(d):
    return pairs(lambda y, c, z, x: ((y + d) % 4, c, z, x))


CORE_SWAP = pairs(lambda y, c, z, x: (y, 1 - c, z, x))

def send(value, route):
    return lax.ppermute(value, ALL, route)


def vmem():
    return pl.BlockSpec(memory_space=pltpu.VMEM)


def grant(mib):
    return pltpu.CompilerParams(vmem_limit_bytes=mib * 1024 * 1024)


def order_projectors(where, projectors):
    def body(where_ref, pq_ref, pk_ref, pv_ref, out_ref):
        core, own = where_ref[0], where_ref[1]
        for n, d in enumerate(ORDER):
            at = lax.broadcasted_iota(jnp.int32, (BLOCK, PROJECT_RANK), 0)
            rank = lax.broadcasted_iota(jnp.int32, (BLOCK, PROJECT_RANK), 1)
            outer, inner = at // RANK_ROWS, at % RANK_ROWS
            a = (own + d) % 4
            straight = a * BLOCK + at
            crossed = outer * BLOCK + a * RANK_ROWS + inner
            wanted = jnp.where(core == 0, straight, crossed)
            pick = jnp.where(rank == wanted, 1.0, 0.0).astype(BF16)
            for m, p_ref in enumerate((pq_ref, pk_ref, pv_ref)):
                rows = lax.dot_general(
                    pick, p_ref[...], (((1,), (1,)), ((), ())), preferred_element_type=F32
                )
                out_ref[m, n * BLOCK : (n + 1) * BLOCK, :] = rows.astype(BF16)

    return pl.pallas_call(
        body,
        grid_spec=pltpu.PrefetchScalarGridSpec(
            num_scalar_prefetch=1,
            grid=(1,),
            in_specs=[vmem()] * 3,
            out_specs=vmem(),
        ),
        out_shape=jax.ShapeDtypeStruct((3, PROJECT_RANK, ROWS), BF16),
        compiler_params=grant(12),
        name="order_projectors",
    )(where, *projectors)


def copies(half, core, grad_refs, into, semaphores):
    blocks = []
    for y in range(4):
        block = []
        for m, low, wide, at in SEGMENTS[half]:
            start = pl.multiple_of((2 * y + core) * (WK if m else WQ) + low, 128)
            block.append(
                pltpu.make_async_copy(
                    grad_refs[m].at[:, pl.ds(start, wide)],
                    into.at[:, pl.ds(y * HALF + at, wide)],
                    semaphores.at[y * len(SEGMENTS[half]) + len(block)],
                )
            )
        blocks.append(block)
    return blocks


def take_columns(half, grads):
    def body(q_ref, k_ref, v_ref, out_ref, semaphores):
        other = 1 - lax.axis_index("dp_1")
        blocks = copies(half, other, (q_ref, k_ref, v_ref), out_ref, semaphores)
        for block in blocks:
            for copy in block:
                copy.start()
        for block in blocks:
            for copy in block:
                copy.wait()

    return pl.pallas_call(
        body,
        in_specs=[pl.BlockSpec(memory_space=pltpu.HBM)] * 3,
        out_specs=vmem(),
        out_shape=jax.ShapeDtypeStruct((ROWS, 4 * HALF), BF16),
        scratch_shapes=[pltpu.SemaphoreType.DMA((4 * len(SEGMENTS[half]),))],
        compiler_params=grant(8),
        name="take_columns",
    )(*grads)


def project(half, transposed, grads, received):
    def body(t_ref, other_ref, q_ref, k_ref, v_ref, *rest):
        outs, scale_ref, own, semaphores = rest[:4], rest[4], rest[5], rest[6]
        core = lax.axis_index("dp_1")
        blocks = copies(half, core, (q_ref, k_ref, v_ref), own, semaphores)
        for block in blocks:
            for copy in block:
                copy.start()
        largest = [jnp.zeros((1, 128), F32)] * 3
        for y, block in enumerate(blocks):
            for copy in block:
                copy.wait()
            for m, low, wide, at in SEGMENTS[half]:
                span = slice(y * HALF + at, y * HALF + at + wide)
                product = jnp.dot(t_ref[m], own[:, span], preferred_element_type=F32)
                product += jnp.dot(t_ref[m], other_ref[:, span], preferred_element_type=F32)
                for n in range(4):
                    piece = product[n * BLOCK : (n + 1) * BLOCK]
                    outs[n][:, span] = piece
                    if n < 3:
                        tall = jnp.max(jnp.abs(piece), axis=0, keepdims=True)
                        for k in range(0, wide, 128):
                            largest[n] = jnp.maximum(largest[n], tall[:, k : k + 128])
        for n in range(3):
            peak = jnp.maximum(jnp.max(largest[n], axis=1, keepdims=True), 1e-30)
            scale = jnp.clip(8192.0 / peak, 0.03125, 32768.0).astype(BF16).astype(F32)
            scale_ref[8 * n : 8 * n + 8, :] = jnp.broadcast_to(scale, (8, 128))
            outs[n][:, 4 * HALF :] = jnp.ones((BLOCK, 128), F32)

    shapes = [(BLOCK, 4 * HALF + 128)] * 3 + [(BLOCK, 4 * HALF), (24, 128)]
    return pl.pallas_call(
        body,
        in_specs=[vmem(), vmem(), *[pl.BlockSpec(memory_space=pltpu.HBM)] * 3],
        out_specs=[vmem()] * 5,
        out_shape=[jax.ShapeDtypeStruct(s, F32) for s in shapes],
        scratch_shapes=[
            pltpu.VMEM((ROWS, 4 * HALF), BF16),
            pltpu.SemaphoreType.DMA((4 * len(SEGMENTS[half]),)),
        ],
        compiler_params=grant(24),
        name="project",
    )(transposed, received, *grads)


def finish_sum(halves):
    def body(*refs):
        sum_ref, square_ref = refs[8], refs[9]
        for h in range(2):
            a, b, c, d = (ref[...] for ref in refs[4 * h : 4 * h + 4])
            sum_ref[:, h * HALF : (h + 1) * HALF] = (a + b) + (c + d)
        total = sum_ref[...]
        square_ref[...] = jnp.broadcast_to(jnp.sum(total * total, keepdims=True), (8, 128))

    return pl.pallas_call(
        body,
        in_specs=[vmem()] * 8,
        out_specs=[vmem()] * 2,
        out_shape=[
            jax.ShapeDtypeStruct((RANK_ROWS, WIDTH), F32),
            jax.ShapeDtypeStruct((8, 128), F32),
        ],
        compiler_params=grant(4),
        name="finish_sum",
    )(*halves[0], *halves[1])


def adam(projected, square_sum, avgs, squares):
    threshold = math.sqrt(PROJECT_RANK * (QUERY_OUTPUTS + 2 * KEY_VALUE_OUTS))
    correct_one = 1.0 - 0.9**STEP
    correct_two = 1.0 - 0.95**STEP

    def body(p_ref, s_ref, *rest):
        avg_refs, sq_refs = rest[:3], rest[3:6]
        new_avg_refs, new_sq_refs, update_ref = rest[6:9], rest[9:12], rest[12]
        clip = jnp.minimum(1.0, threshold / jnp.sqrt(s_ref[0:1, 0:1] + 1e-06))
        at = 0
        for m in range(3):
            wide = avg_refs[m].shape[1]
            scaled = clip * p_ref[:, at : at + wide]
            new_avg = 0.9 * avg_refs[m][...] + 0.1 * scaled
            new_sq = 0.95 * sq_refs[m][...] + 0.05 * scaled * scaled
            new_avg_refs[m][...] = new_avg
            new_sq_refs[m][...] = new_sq
            update = new_avg / correct_one / (jnp.sqrt(new_sq / correct_two) + 1e-08)
            update_ref[:, at : at + wide] = update.astype(BF16)
            at += wide

    like = [jax.ShapeDtypeStruct(a.shape, F32) for a in avgs]
    return pl.pallas_call(
        body,
        out_shape=[*like, *like, jax.ShapeDtypeStruct((RANK_ROWS, WIDTH), BF16)],
        compiler_params=grant(4),
        name="adam",
    )(projected, square_sum, *avgs, *squares)


def apply_updates(where, gathered, projectors, weights, comps):
    tile = 128

    def body(where_ref, *refs):
        parts, (pq, pk, pv), ws, cs = refs[:4], refs[4:7], refs[7:10], refs[10:13]
        outs, update = refs[13:16], refs[16]

        @pl.when(pl.program_id(0) == 0)
        def _():
            core, first, second = where_ref[0], where_ref[1], where_ref[2]
            for d in range(4):
                for k in range(4):
                    far = (first + 4 - d) % 4
                    near = (second + 4 - k) % 4
                    z = jnp.where(core == 0, far, near)
                    x = jnp.where(core == 0, near, far)
                    at = pl.multiple_of(z * BLOCK + x * RANK_ROWS, RANK_ROWS)
                    update[pl.ds(at, RANK_ROWS), :] = parts[d][k * RANK_ROWS : (k + 1) * RANK_ROWS, :]

        at = 0
        rows = pl.ds(pl.multiple_of(pl.program_id(0) * tile, tile), tile)
        for m, p_ref in enumerate((pq, pk, pv)):
            wide = ws[m].shape[1]
            product = jnp.dot(p_ref[rows, :], update[:, at : at + wide], preferred_element_type=F32)
            outs[m][...] = ws[m][rows, :].astype(F32) + (-0.04 * product + cs[m][rows, :].astype(F32))
            at += wide

    def rows(i, where):
        return (i, 0)

    tall = [pl.BlockSpec((tile, w.shape[1]), rows) for w in weights]
    return pl.pallas_call(
        body,
        grid_spec=pltpu.PrefetchScalarGridSpec(
            num_scalar_prefetch=1,
            grid=(ROWS // tile,),
            in_specs=[vmem()] * 13,
            out_specs=tall,
            scratch_shapes=[pltpu.VMEM((PROJECT_RANK, WIDTH), BF16)],
        ),
        out_shape=[jax.ShapeDtypeStruct(w.shape, F32) for w in weights],
        compiler_params=grant(16),
        name="apply_updates",
    )(where, *gathered, *projectors, *weights, *comps)


def shards(
    grad_q,
    grad_k,
    grad_v,
    proj_q,
    proj_k,
    proj_v,
    weight_q,
    key_weight_matrix,
    value_weight_matrix,
    comp_q,
    key_compensation,
    value_compensation,
    avg_q,
    key_first_moment,
    value_first_moment,
    sq_q,
    key_second_moment,
    value_second_moment,
):
    grads = tuple(
        pltpu.with_memory_space_constraint(g[0], pltpu.HBM) for g in (grad_q, grad_k, grad_v)
    )
    projectors = (proj_q, proj_k, proj_v)
    y, core, z, x = (lax.axis_index(name) for name in ALL)
    first = jnp.where(core == 0, z, x)
    second = jnp.where(core == 0, x, z)
    where = jnp.stack([core, first, second]).astype(jnp.int32)

    received = [send(take_columns(half, grads), CORE_SWAP) for half in range(2)]
    transposed = order_projectors(where, projectors)

    def reduce_half(half):
        *pieces, own, scales = project(half, transposed, grads, received[half])
        arrived = [
            send((piece * scales[8 * n, 0]).astype(F16), along_first(d))
            for n, (d, piece) in enumerate(zip(ORDER, pieces))
        ]

        def rank_rows(b):
            at = b * RANK_ROWS
            total = lax.dynamic_slice_in_dim(own, at, RANK_ROWS, axis=0)
            for part in arrived:
                scale = part[0, 4 * HALF].astype(F32)
                rows = lax.dynamic_slice_in_dim(part, at, RANK_ROWS, axis=0)[:, : 4 * HALF]
                total = total + rows.astype(F32) / scale
            return total

        parts = {d: rank_rows((second + d) % 4) for d in ORDER}
        arrived = [send(parts[d], along_second(d)) for d in ORDER[:3]]

        def columns(b):
            total = lax.dynamic_slice_in_dim(parts[0], b * HALF, HALF, axis=1)
            for part in arrived:
                total = total + lax.dynamic_slice_in_dim(part, b * HALF, HALF, axis=1)
            return total

        blocks = {d: columns((y + d) % 4) for d in ORDER}
        return [blocks[0], *[send(blocks[d], along_y(d)) for d in ORDER[:3]]]

    projected, square_sum = finish_sum([reduce_half(half) for half in range(2)])
    square_sum = square_sum + send(square_sum, CORE_SWAP)
    for along in (along_y, along_first, along_second):
        a, b, c = (send(square_sum, along(d)) for d in ORDER[:3])
        square_sum = (square_sum + a) + (b + c)

    *moments, update = adam(
        projected,
        square_sum,
        (avg_q, key_first_moment, value_first_moment),
        (sq_q, key_second_moment, value_second_moment),
    )

    held = jnp.concatenate([update, *[send(update, along_second(d)) for d in (1, 2, 3)]], axis=0)
    gathered = [held, *[send(held, along_first(d)) for d in (1, 2, 3)]]
    new_weights = apply_updates(
        where,
        gathered,
        projectors,
        (weight_q, key_weight_matrix, value_weight_matrix),
        (comp_q, key_compensation, value_compensation),
    )
    return (*new_weights, *moments)


def solution(mesh):
    split = Mesh(mesh.devices.reshape(4, 2, 4, 4), ALL)
    return jax.shard_map(
        shards,
        mesh=split,
        in_specs=(*[P(DP, FSDP, None)] * 3, *[P(FSDP, None)] * 3, *[P(FSDP, DP)] * 12),
        out_specs=(*[P(FSDP, DP)] * 9,),
        check_vma=False,
    )
```

```python
import math

import jax
import jax.numpy as jnp
from jax import lax
from jax.experimental import pallas as pl
from jax.experimental.pallas import tpu as pltpu
from jax.sharding import Mesh
from jax.sharding import PartitionSpec as P

QUERY_OUTPUTS = 8192
KEY_VALUE_OUTS = 1024
PROJECT_RANK = 512
STEP = 10
DP = ("dp_0", "dp_1")
FSDP = ("fsdp_0", "fsdp_1")
ALL = ("dp_0", "dp_1", "fsdp_0", "fsdp_1")

ROWS = 512
RANK_ROWS = 32
BLOCK = 128
WQ, WK = 1024, 128
WIDTH = WQ + 2 * WK
HALF = WIDTH // 2
ORDER = (1, 3, 2, 0)
SEGMENTS = (((0, 0, HALF, 0),), ((0, HALF, WQ - HALF, 0), (1, 0, WK, WQ - HALF), (2, 0, WK, WQ - HALF + WK)))


F32 = jnp.float32
BF16 = jnp.bfloat16
F16 = jnp.float16


def pairs(move):
    found = []
    for y in range(4):
        for c in range(2):
            for z in range(4):
                for x in range(4):
                    ty, tc, tz, tx = move(y, c, z, x)
                    source = ((y * 2 + c) * 4 + z) * 4 + x
                    found.append((source, ((ty * 2 + tc) * 4 + tz) * 4 + tx))
    return found


def along_first(d):
    return pairs(lambda y, c, z, x: (y, c, (z + d) % 4, x) if c == 0 else (y, c, z, (x + d) % 4))


def along_second(d):
    return pairs(lambda y, c, z, x: (y, c, z, (x + d) % 4) if c == 0 else (y, c, (z + d) % 4, x))


def along_y(d):
    return pairs(lambda y, c, z, x: ((y + d) % 4, c, z, x))


CORE_SWAP = pairs(lambda y, c, z, x: (y, 1 - c, z, x))

def send(value, route):
    return lax.ppermute(value, ALL, route)


def vmem():
    return pl.BlockSpec(memory_space=pltpu.VMEM)


def grant(mib):
    return pltpu.CompilerParams(vmem_limit_bytes=mib * 1024 * 1024)


def order_projectors(where, projectors):
    def body(where_ref, pq_ref, pk_ref, pv_ref, out_ref):
        core, own = where_ref[0], where_ref[1]
        for n, d in enumerate(ORDER):
            at = lax.broadcasted_iota(jnp.int32, (BLOCK, PROJECT_RANK), 0)
            rank = lax.broadcasted_iota(jnp.int32, (BLOCK, PROJECT_RANK), 1)
            outer, inner = at // RANK_ROWS, at % RANK_ROWS
            a = (own + d) % 4
            straight = a * BLOCK + at
            crossed = outer * BLOCK + a * RANK_ROWS + inner
            wanted = jnp.where(core == 0, straight, crossed)
            pick = jnp.where(rank == wanted, 1.0, 0.0).astype(BF16)
            for m, p_ref in enumerate((pq_ref, pk_ref, pv_ref)):
                rows = lax.dot_general(
                    pick, p_ref[...], (((1,), (1,)), ((), ())), preferred_element_type=F32
                )
                for k in range(2):
                    out_ref[m, n * BLOCK : (n + 1) * BLOCK, k * ROWS : (k + 1) * ROWS] = rows.astype(BF16)

    return pl.pallas_call(
        body,
        grid_spec=pltpu.PrefetchScalarGridSpec(
            num_scalar_prefetch=1,
            grid=(1,),
            in_specs=[vmem()] * 3,
            out_specs=vmem(),
        ),
        out_shape=jax.ShapeDtypeStruct((3, PROJECT_RANK, 2 * ROWS), BF16),
        compiler_params=grant(12),
        name="order_projectors",
    )(where, *projectors)


def copies(half, core, grad_refs, into, semaphores):
    blocks = []
    for y in range(4):
        block = []
        for m, low, wide, at in SEGMENTS[half]:
            start = pl.multiple_of((2 * y + core) * (WK if m else WQ) + low, 128)
            block.append(
                pltpu.make_async_copy(
                    grad_refs[m].at[:, pl.ds(start, wide)],
                    into.at[:, pl.ds(y * HALF + at, wide)],
                    semaphores.at[y * len(SEGMENTS[half]) + len(block)],
                )
            )
        blocks.append(block)
    return blocks


def take_columns(half, grads):
    def body(q_ref, k_ref, v_ref, out_ref, semaphores):
        other = 1 - lax.axis_index("dp_1")
        blocks = copies(half, other, (q_ref, k_ref, v_ref), out_ref, semaphores)
        for block in blocks:
            for copy in block:
                copy.start()
        for block in blocks:
            for copy in block:
                copy.wait()

    return pl.pallas_call(
        body,
        in_specs=[pl.BlockSpec(memory_space=pltpu.HBM)] * 3,
        out_specs=pl.BlockSpec(memory_space=pltpu.HBM),
        out_shape=jax.ShapeDtypeStruct((ROWS, 4 * HALF), BF16),
        scratch_shapes=[pltpu.SemaphoreType.DMA((4 * len(SEGMENTS[half]),))],
        compiler_params=grant(8),
        name="take_columns",
    )(*grads)


def power_of_two(peak):
    scale = jnp.full(peak.shape, 2.0**-5, F32)
    for k in range(-4, 15):
        scale = jnp.where(peak * 2.0**k <= 16384.0, 2.0**k, scale)
    return scale


def project(half, transposed, grads, received):
    parts = len(SEGMENTS[half])

    def body(t_ref, other_ref, q_ref, k_ref, v_ref, *rest):
        outs, both, semaphores, other_semaphores = rest[:4], rest[4], rest[5], rest[6]
        core = lax.axis_index("dp_1")
        blocks = copies(half, core, (q_ref, k_ref, v_ref), both.at[:ROWS], semaphores)
        for y, block in enumerate(blocks):
            span = pl.ds(y * HALF, HALF)
            block.append(
                pltpu.make_async_copy(
                    other_ref.at[:, span], both.at[pl.ds(ROWS, ROWS), span], other_semaphores.at[y]
                )
            )
            for copy in block:
                copy.start()
        largest = [jnp.zeros((8, 128), F32)] * 3
        for y, block in enumerate(blocks):
            for copy in block:
                copy.wait()
            for m, low, wide, at in SEGMENTS[half]:
                span = slice(y * HALF + at, y * HALF + at + wide)
                product = jnp.dot(t_ref[m], both[:, span], preferred_element_type=F32)
                for n in range(4):
                    piece = product[n * BLOCK : (n + 1) * BLOCK]
                    outs[n][:, span] = piece
                    if n < 3:
                        tall = jnp.abs(piece)
                        for r in range(0, BLOCK, 8):
                            for k in range(0, wide, 128):
                                largest[n] = jnp.maximum(largest[n], tall[r : r + 8, k : k + 128])
        for n in range(3):
            peak = jnp.max(jnp.max(largest[n], axis=0, keepdims=True), axis=1, keepdims=True)
            scale = power_of_two(peak)
            outs[n][:, : 4 * HALF] = outs[n][:, : 4 * HALF] * scale
            outs[n][:, 4 * HALF :] = jnp.broadcast_to(1.0 / scale, (BLOCK, 128))

    shapes = [(BLOCK, 4 * HALF + 128)] * 3 + [(BLOCK, 4 * HALF)]
    return pl.pallas_call(
        body,
        in_specs=[vmem(), *[pl.BlockSpec(memory_space=pltpu.HBM)] * 4],
        out_specs=[vmem()] * 4,
        out_shape=[jax.ShapeDtypeStruct(s, F32) for s in shapes],
        scratch_shapes=[
            pltpu.VMEM((2 * ROWS, 4 * HALF), BF16),
            pltpu.SemaphoreType.DMA((4 * parts,)),
            pltpu.SemaphoreType.DMA((4,)),
        ],
        compiler_params=grant(18),
        name="project",
    )(transposed, pltpu.with_memory_space_constraint(received, pltpu.HBM), *grads)


def finish_sum(halves):
    def body(*refs):
        sum_ref, square_ref = refs[8], refs[9]
        for h in range(2):
            a, b, c, d = (ref[...] for ref in refs[4 * h : 4 * h + 4])
            sum_ref[:, h * HALF : (h + 1) * HALF] = (a + b) + (c + d)
        total = sum_ref[...]
        square_ref[...] = jnp.broadcast_to(jnp.sum(total * total, keepdims=True), (8, 128))

    return pl.pallas_call(
        body,
        in_specs=[vmem()] * 8,
        out_specs=[vmem()] * 2,
        out_shape=[
            jax.ShapeDtypeStruct((RANK_ROWS, WIDTH), F32),
            jax.ShapeDtypeStruct((8, 128), F32),
        ],
        compiler_params=grant(4),
        name="finish_sum",
    )(*halves[0], *halves[1])


def adam(projected, square_sum, avgs, squares):
    threshold = math.sqrt(PROJECT_RANK * (QUERY_OUTPUTS + 2 * KEY_VALUE_OUTS))
    correct_one = 1.0 - 0.9**STEP
    correct_two = 1.0 - 0.95**STEP

    def body(p_ref, s_ref, *rest):
        avg_refs, sq_refs = rest[:3], rest[3:6]
        new_avg_refs, new_sq_refs, update_ref = rest[6:9], rest[9:12], rest[12]
        clip = jnp.minimum(1.0, threshold / jnp.sqrt(s_ref[0:1, 0:1] + 1e-06))
        at = 0
        for m in range(3):
            wide = avg_refs[m].shape[1]
            scaled = clip * p_ref[:, at : at + wide]
            new_avg = 0.9 * avg_refs[m][...] + 0.1 * scaled
            new_sq = 0.95 * sq_refs[m][...] + 0.05 * scaled * scaled
            new_avg_refs[m][...] = new_avg
            new_sq_refs[m][...] = new_sq
            update = new_avg / correct_one / (jnp.sqrt(new_sq / correct_two) + 1e-08)
            update_ref[:, at : at + wide] = update.astype(BF16)
            at += wide

    like = [jax.ShapeDtypeStruct(a.shape, F32) for a in avgs]
    return pl.pallas_call(
        body,
        out_shape=[*like, *like, jax.ShapeDtypeStruct((RANK_ROWS, WIDTH), BF16)],
        compiler_params=grant(4),
        name="adam",
    )(projected, square_sum, *avgs, *squares)


def apply_updates(where, gathered, projectors, weights, comps):
    tile = 128

    def body(where_ref, *refs):
        parts, (pq, pk, pv), ws, cs = refs[:4], refs[4:7], refs[7:10], refs[10:13]
        outs, update = refs[13:16], refs[16]

        @pl.when(pl.program_id(0) == 0)
        def _():
            core, first, second = where_ref[0], where_ref[1], where_ref[2]
            for d in range(4):
                for k in range(4):
                    far = (first + 4 - d) % 4
                    near = (second + 4 - k) % 4
                    z = jnp.where(core == 0, far, near)
                    x = jnp.where(core == 0, near, far)
                    at = pl.multiple_of(z * BLOCK + x * RANK_ROWS, RANK_ROWS)
                    update[pl.ds(at, RANK_ROWS), :] = parts[d][k * RANK_ROWS : (k + 1) * RANK_ROWS, :]

        at = 0
        rows = pl.ds(pl.multiple_of(pl.program_id(0) * tile, tile), tile)
        for m, p_ref in enumerate((pq, pk, pv)):
            wide = ws[m].shape[1]
            product = jnp.dot(p_ref[rows, :], update[:, at : at + wide], preferred_element_type=F32)
            outs[m][...] = ws[m][rows, :].astype(F32) + (-0.04 * product + cs[m][rows, :].astype(F32))
            at += wide

    def rows(i, where):
        return (i, 0)

    tall = [pl.BlockSpec((tile, w.shape[1]), rows) for w in weights]
    return pl.pallas_call(
        body,
        grid_spec=pltpu.PrefetchScalarGridSpec(
            num_scalar_prefetch=1,
            grid=(ROWS // tile,),
            in_specs=[vmem()] * 13,
            out_specs=tall,
            scratch_shapes=[pltpu.VMEM((PROJECT_RANK, WIDTH), BF16)],
        ),
        out_shape=[jax.ShapeDtypeStruct(w.shape, F32) for w in weights],
        compiler_params=grant(16),
        name="apply_updates",
    )(where, *gathered, *projectors, *weights, *comps)


def shards(
    grad_q,
    grad_k,
    grad_v,
    proj_q,
    proj_k,
    proj_v,
    weight_q,
    key_weight_matrix,
    value_weight_matrix,
    comp_q,
    key_compensation,
    value_compensation,
    avg_q,
    key_first_moment,
    value_first_moment,
    sq_q,
    key_second_moment,
    value_second_moment,
):
    grads = tuple(
        pltpu.with_memory_space_constraint(g[0], pltpu.HBM) for g in (grad_q, grad_k, grad_v)
    )
    projectors = (proj_q, proj_k, proj_v)
    y, core, z, x = (lax.axis_index(name) for name in ALL)
    first = jnp.where(core == 0, z, x)
    second = jnp.where(core == 0, x, z)
    where = jnp.stack([core, first, second]).astype(jnp.int32)

    received = [send(take_columns(half, grads), CORE_SWAP) for half in range(2)]
    transposed = order_projectors(where, projectors)

    def reduce_half(half):
        *pieces, own = project(half, transposed, grads, received[half])
        arrived = [send(piece.astype(F16), along_first(d)) for d, piece in zip(ORDER, pieces)]

        def rank_rows(b):
            at = b * RANK_ROWS
            total = lax.dynamic_slice_in_dim(own, at, RANK_ROWS, axis=0)
            for part in arrived:
                rows = lax.dynamic_slice_in_dim(part, at, RANK_ROWS, axis=0).astype(F32)
                total = total + rows[:, : 4 * HALF] * rows[:, 4 * HALF : 4 * HALF + 1]
            return total

        parts = {d: rank_rows((second + d) % 4) for d in ORDER}
        arrived = [send(parts[d], along_second(d)) for d in ORDER[:3]]

        def columns(b):
            total = lax.dynamic_slice_in_dim(parts[0], b * HALF, HALF, axis=1)
            for part in arrived:
                total = total + lax.dynamic_slice_in_dim(part, b * HALF, HALF, axis=1)
            return total

        blocks = {d: columns((y + d) % 4) for d in ORDER}
        return [blocks[0], *[send(blocks[d], along_y(d)) for d in ORDER[:3]]]

    projected, square_sum = finish_sum([reduce_half(half) for half in range(2)])
    square_sum = square_sum + send(square_sum, CORE_SWAP)
    for along in (along_y, along_first, along_second):
        a, b, c = (send(square_sum, along(d)) for d in ORDER[:3])
        square_sum = (square_sum + a) + (b + c)

    *moments, update = adam(
        projected,
        square_sum,
        (avg_q, key_first_moment, value_first_moment),
        (sq_q, key_second_moment, value_second_moment),
    )

    held = jnp.concatenate([update, *[send(update, along_second(d)) for d in (1, 2, 3)]], axis=0)
    gathered = [held, *[send(held, along_first(d)) for d in (1, 2, 3)]]
    new_weights = apply_updates(
        where,
        gathered,
        projectors,
        (weight_q, key_weight_matrix, value_weight_matrix),
        (comp_q, key_compensation, value_compensation),
    )
    return (*new_weights, *moments)


def solution(mesh):
    split = Mesh(mesh.devices.reshape(4, 2, 4, 4), ALL)
    return jax.shard_map(
        shards,
        mesh=split,
        in_specs=(*[P(DP, FSDP, None)] * 3, *[P(FSDP, None)] * 3, *[P(FSDP, DP)] * 12),
        out_specs=(*[P(FSDP, DP)] * 9,),
        check_vma=False,
    )
```

```python
import math

import jax
import jax.numpy as jnp
from jax import lax
from jax.experimental import pallas as pl
from jax.experimental.pallas import tpu as pltpu
from jax.sharding import Mesh
from jax.sharding import PartitionSpec as P

QUERY_OUTPUTS = 8192
KEY_VALUE_OUTS = 1024
PROJECT_RANK = 512
STEP = 10
DP = ("dp_0", "dp_1")
FSDP = ("fsdp_0", "fsdp_1")
ALL = ("dp_0", "dp_1", "fsdp_0", "fsdp_1")

ROWS = 512
RANK_ROWS = 32
BLOCK = 128
WQ, WK = 1024, 128
WIDTH = WQ + 2 * WK
HALF = WIDTH // 2
ORDER = (1, 3, 2, 0)
SEGMENTS = (((0, 0, HALF, 0),), ((0, HALF, WQ - HALF, 0), (1, 0, WK, WQ - HALF), (2, 0, WK, WQ - HALF + WK)))


F32 = jnp.float32
BF16 = jnp.bfloat16
F16 = jnp.float16


def pairs(move):
    found = []
    for y in range(4):
        for c in range(2):
            for z in range(4):
                for x in range(4):
                    ty, tc, tz, tx = move(y, c, z, x)
                    source = ((y * 2 + c) * 4 + z) * 4 + x
                    found.append((source, ((ty * 2 + tc) * 4 + tz) * 4 + tx))
    return found


def along_first(d):
    return pairs(lambda y, c, z, x: (y, c, (z + d) % 4, x) if c == 0 else (y, c, z, (x + d) % 4))


def along_second(d):
    return pairs(lambda y, c, z, x: (y, c, z, (x + d) % 4) if c == 0 else (y, c, (z + d) % 4, x))


def along_y(d):
    return pairs(lambda y, c, z, x: ((y + d) % 4, c, z, x))


CORE_SWAP = pairs(lambda y, c, z, x: (y, 1 - c, z, x))

def send(value, route):
    return lax.ppermute(value, ALL, route)


def vmem():
    return pl.BlockSpec(memory_space=pltpu.VMEM)


def grant(mib):
    return pltpu.CompilerParams(vmem_limit_bytes=mib * 1024 * 1024)


def order_projectors(projectors):
    def body(pq_hbm, pk_hbm, pv_hbm, out_ref, pq_ref, pk_ref, pv_ref, semaphores):
        arriving = [
            pltpu.make_async_copy(source, target, semaphores.at[m])
            for m, (source, target) in enumerate(
                ((pq_hbm, pq_ref), (pk_hbm, pk_ref), (pv_hbm, pv_ref))
            )
        ]
        for copy in arriving:
            copy.start()
        for copy in arriving:
            copy.wait()
        core = lax.axis_index("dp_1")
        own = jnp.where(core == 0, lax.axis_index("fsdp_0"), lax.axis_index("fsdp_1"))
        for n, d in enumerate(ORDER):
            at = lax.broadcasted_iota(jnp.int32, (BLOCK, PROJECT_RANK), 0)
            rank = lax.broadcasted_iota(jnp.int32, (BLOCK, PROJECT_RANK), 1)
            outer, inner = at // RANK_ROWS, at % RANK_ROWS
            a = (own + d) % 4
            straight = a * BLOCK + at
            crossed = outer * BLOCK + a * RANK_ROWS + inner
            wanted = jnp.where(core == 0, straight, crossed)
            pick = jnp.where(rank == wanted, 1.0, 0.0).astype(BF16)
            for m, p_ref in enumerate((pq_ref, pk_ref, pv_ref)):
                rows = lax.dot_general(
                    pick, p_ref[...], (((1,), (1,)), ((), ())), preferred_element_type=F32
                )
                for k in range(2):
                    out_ref[m, n * BLOCK : (n + 1) * BLOCK, k * ROWS : (k + 1) * ROWS] = rows.astype(BF16)

    return pl.pallas_call(
        body,
        in_specs=[pl.BlockSpec(memory_space=pltpu.HBM)] * 3,
        out_specs=vmem(),
        out_shape=jax.ShapeDtypeStruct((3, PROJECT_RANK, 2 * ROWS), BF16),
        scratch_shapes=[
            *[pltpu.VMEM((ROWS, PROJECT_RANK), BF16)] * 3,
            pltpu.SemaphoreType.DMA((3,)),
        ],
        compiler_params=grant(12),
        name="order_projectors",
    )(*(pltpu.with_memory_space_constraint(p, pltpu.HBM) for p in projectors))


def copies(half, core, grad_refs, into, semaphores):
    blocks = []
    for y in range(4):
        block = []
        for m, low, wide, at in SEGMENTS[half]:
            start = pl.multiple_of((2 * y + core) * (WK if m else WQ) + low, 128)
            block.append(
                pltpu.make_async_copy(
                    grad_refs[m].at[:, pl.ds(start, wide)],
                    into.at[:, pl.ds(y * HALF + at, wide)],
                    semaphores.at[y * len(SEGMENTS[half]) + len(block)],
                )
            )
        blocks.append(block)
    return blocks


def take_columns(half, grads):
    parts = len(SEGMENTS[half])

    def body(q_ref, k_ref, v_ref, out_ref, held, semaphores, out_semaphores):
        other = 1 - lax.axis_index("dp_1")
        blocks = copies(half, other, (q_ref, k_ref, v_ref), held, semaphores)
        for block in blocks:
            for copy in block:
                copy.start()
        leaving = []
        for y, block in enumerate(blocks):
            for copy in block:
                copy.wait()
            span = pl.ds(y * HALF, HALF)
            copy = pltpu.make_async_copy(held.at[:, span], out_ref.at[:, span], out_semaphores.at[y])
            copy.start()
            leaving.append(copy)
        for copy in leaving:
            copy.wait()

    return pl.pallas_call(
        body,
        in_specs=[pl.BlockSpec(memory_space=pltpu.HBM)] * 3,
        out_specs=pl.BlockSpec(memory_space=pltpu.HBM),
        out_shape=jax.ShapeDtypeStruct((ROWS, 4 * HALF), BF16),
        scratch_shapes=[
            pltpu.VMEM((ROWS, 4 * HALF), BF16),
            pltpu.SemaphoreType.DMA((4 * parts,)),
            pltpu.SemaphoreType.DMA((4,)),
        ],
        compiler_params=grant(8),
        name="take_columns",
    )(*grads)


def power_of_two(peak):
    scale = jnp.full(peak.shape, 2.0**-5, F32)
    for k in range(-4, 15):
        scale = jnp.where(peak * 2.0**k <= 16384.0, 2.0**k, scale)
    return scale


def project(half, transposed, grads, received):
    parts = len(SEGMENTS[half])

    def body(t_ref, other_ref, q_ref, k_ref, v_ref, *rest):
        outs, both, semaphores, other_semaphores = rest[:4], rest[4], rest[5], rest[6]
        core = lax.axis_index("dp_1")
        blocks = copies(half, core, (q_ref, k_ref, v_ref), both.at[:ROWS], semaphores)
        for y, block in enumerate(blocks):
            span = pl.ds(y * HALF, HALF)
            block.append(
                pltpu.make_async_copy(
                    other_ref.at[:, span], both.at[pl.ds(ROWS, ROWS), span], other_semaphores.at[y]
                )
            )
            for copy in block:
                copy.start()
        largest = [jnp.zeros((8, 128), F32)] * 3
        for y, block in enumerate(blocks):
            for copy in block:
                copy.wait()
            for m, low, wide, at in SEGMENTS[half]:
                span = slice(y * HALF + at, y * HALF + at + wide)
                product = jnp.dot(t_ref[m], both[:, span], preferred_element_type=F32)
                for n in range(4):
                    piece = product[n * BLOCK : (n + 1) * BLOCK]
                    outs[n][:, span] = piece
                    if n < 3:
                        tall = jnp.abs(piece)
                        for r in range(0, BLOCK, 8):
                            for k in range(0, wide, 128):
                                largest[n] = jnp.maximum(largest[n], tall[r : r + 8, k : k + 128])
        for n in range(3):
            peak = jnp.max(jnp.max(largest[n], axis=0, keepdims=True), axis=1, keepdims=True)
            scale = power_of_two(peak)
            outs[n][:, : 4 * HALF] = outs[n][:, : 4 * HALF] * scale
            outs[n][:, 4 * HALF :] = jnp.broadcast_to(1.0 / scale, (BLOCK, 128))

    shapes = [(BLOCK, 4 * HALF + 128)] * 3 + [(BLOCK, 4 * HALF)]
    return pl.pallas_call(
        body,
        in_specs=[vmem(), pl.BlockSpec(memory_space=pl.ANY), *[pl.BlockSpec(memory_space=pltpu.HBM)] * 3],
        out_specs=[vmem()] * 4,
        out_shape=[jax.ShapeDtypeStruct(s, F32) for s in shapes],
        scratch_shapes=[
            pltpu.VMEM((2 * ROWS, 4 * HALF), BF16),
            pltpu.SemaphoreType.DMA((4 * parts,)),
            pltpu.SemaphoreType.DMA((4,)),
        ],
        compiler_params=grant(18),
        name="project",
    )(transposed, received, *grads)


def finish_sum(halves):
    def body(*refs):
        sum_ref, square_ref = refs[8], refs[9]
        for h in range(2):
            a, b, c, d = (ref[...] for ref in refs[4 * h : 4 * h + 4])
            sum_ref[:, h * HALF : (h + 1) * HALF] = (a + b) + (c + d)
        total = sum_ref[...]
        square_ref[...] = jnp.broadcast_to(jnp.sum(total * total, keepdims=True), (8, 128))

    return pl.pallas_call(
        body,
        in_specs=[vmem()] * 8,
        out_specs=[vmem()] * 2,
        out_shape=[
            jax.ShapeDtypeStruct((RANK_ROWS, WIDTH), F32),
            jax.ShapeDtypeStruct((8, 128), F32),
        ],
        compiler_params=grant(4),
        name="finish_sum",
    )(*halves[0], *halves[1])


def adam(projected, square_sum, avgs, squares):
    threshold = math.sqrt(PROJECT_RANK * (QUERY_OUTPUTS + 2 * KEY_VALUE_OUTS))
    correct_one = 1.0 - 0.9**STEP
    correct_two = 1.0 - 0.95**STEP

    def body(p_ref, s_ref, *rest):
        avg_refs, sq_refs = rest[:3], rest[3:6]
        new_avg_refs, new_sq_refs, update_ref = rest[6:9], rest[9:12], rest[12]
        clip = jnp.minimum(1.0, threshold / jnp.sqrt(s_ref[0:1, 0:1] + 1e-06))
        at = 0
        for m in range(3):
            wide = avg_refs[m].shape[1]
            scaled = clip * p_ref[:, at : at + wide]
            new_avg = 0.9 * avg_refs[m][...] + 0.1 * scaled
            new_sq = 0.95 * sq_refs[m][...] + 0.05 * scaled * scaled
            new_avg_refs[m][...] = new_avg
            new_sq_refs[m][...] = new_sq
            update = new_avg / correct_one / (jnp.sqrt(new_sq / correct_two) + 1e-08)
            update_ref[:, at : at + wide] = update.astype(BF16)
            at += wide

    like = [jax.ShapeDtypeStruct(a.shape, F32) for a in avgs]
    return pl.pallas_call(
        body,
        out_shape=[*like, *like, jax.ShapeDtypeStruct((RANK_ROWS, WIDTH), BF16)],
        compiler_params=grant(4),
        name="adam",
    )(projected, square_sum, *avgs, *squares)


def apply_updates(where, gathered, projectors, weights, comps):
    tile = 128

    def body(where_ref, *refs):
        parts, (pq, pk, pv), ws, cs = refs[:4], refs[4:7], refs[7:10], refs[10:13]
        outs, update = refs[13:16], refs[16]

        @pl.when(pl.program_id(0) == 0)
        def _():
            core, first, second = where_ref[0], where_ref[1], where_ref[2]
            for d in range(4):
                for k in range(4):
                    far = (first + 4 - d) % 4
                    near = (second + 4 - k) % 4
                    z = jnp.where(core == 0, far, near)
                    x = jnp.where(core == 0, near, far)
                    at = pl.multiple_of(z * BLOCK + x * RANK_ROWS, RANK_ROWS)
                    update[pl.ds(at, RANK_ROWS), :] = parts[d][k * RANK_ROWS : (k + 1) * RANK_ROWS, :]

        at = 0
        rows = pl.ds(pl.multiple_of(pl.program_id(0) * tile, tile), tile)
        for m, p_ref in enumerate((pq, pk, pv)):
            wide = ws[m].shape[1]
            product = jnp.dot(p_ref[rows, :], update[:, at : at + wide], preferred_element_type=F32)
            outs[m][...] = ws[m][rows, :].astype(F32) + (-0.04 * product + cs[m][rows, :].astype(F32))
            at += wide

    def rows(i, where):
        return (i, 0)

    tall = [pl.BlockSpec((tile, w.shape[1]), rows) for w in weights]
    return pl.pallas_call(
        body,
        grid_spec=pltpu.PrefetchScalarGridSpec(
            num_scalar_prefetch=1,
            grid=(ROWS // tile,),
            in_specs=[vmem()] * 13,
            out_specs=tall,
            scratch_shapes=[pltpu.VMEM((PROJECT_RANK, WIDTH), BF16)],
        ),
        out_shape=[jax.ShapeDtypeStruct(w.shape, F32) for w in weights],
        compiler_params=grant(16),
        name="apply_updates",
    )(where, *gathered, *projectors, *weights, *comps)


def shards(
    grad_q,
    grad_k,
    grad_v,
    proj_q,
    proj_k,
    proj_v,
    weight_q,
    key_weight_matrix,
    value_weight_matrix,
    comp_q,
    key_compensation,
    value_compensation,
    avg_q,
    key_first_moment,
    value_first_moment,
    sq_q,
    key_second_moment,
    value_second_moment,
):
    grads = tuple(
        pltpu.with_memory_space_constraint(g[0], pltpu.HBM) for g in (grad_q, grad_k, grad_v)
    )
    projectors = (proj_q, proj_k, proj_v)
    y, core, z, x = (lax.axis_index(name) for name in ALL)
    first = jnp.where(core == 0, z, x)
    second = jnp.where(core == 0, x, z)
    where = jnp.stack([core, first, second]).astype(jnp.int32)

    received = [send(take_columns(half, grads), CORE_SWAP) for half in range(2)]
    transposed = order_projectors(projectors)

    def reduce_half(half):
        *pieces, own = project(half, transposed, grads, received[half])
        arrived = [send(piece.astype(F16), along_first(d)) for d, piece in zip(ORDER, pieces)]

        def summed(cut):
            total = cut(own)
            for part in arrived:
                total = total + cut(part).astype(F32) * undo(part, cut)
            return total

        def undo(part, cut):
            return cut(part, scale=True).astype(F32)

        def rank_rows(b):
            def cut(x, scale=False):
                rows = lax.dynamic_slice_in_dim(x, b * RANK_ROWS, RANK_ROWS, axis=0)
                return rows[:, 4 * HALF : 4 * HALF + 1] if scale else rows[:, : 4 * HALF]

            return summed(cut)

        def column_block(b):
            def cut(x, scale=False):
                if scale:
                    return x[:, 4 * HALF : 4 * HALF + 1]
                return lax.dynamic_slice_in_dim(x, b * HALF, HALF, axis=1)

            return summed(cut)

        def regroup(parts, cut):
            total = cut(parts[0])
            for part in parts[1:]:
                total = total + cut(part)
            return total

        if half == 0:
            parts = {d: column_block((y + d) % 4) for d in ORDER}
            parts = [parts[0], *[send(parts[d], along_y(d)) for d in ORDER[:3]]]

            def last(b):
                return regroup(
                    parts, lambda x: lax.dynamic_slice_in_dim(x, b * RANK_ROWS, RANK_ROWS, axis=0)
                )

            blocks = {d: last((second + d) % 4) for d in ORDER}
            return [blocks[0], *[send(blocks[d], along_second(d)) for d in ORDER[:3]]]

        parts = {d: rank_rows((second + d) % 4) for d in ORDER}
        parts = [parts[0], *[send(parts[d], along_second(d)) for d in ORDER[:3]]]

        def last(b):
            return regroup(parts, lambda x: lax.dynamic_slice_in_dim(x, b * HALF, HALF, axis=1))

        blocks = {d: last((y + d) % 4) for d in ORDER}
        return [blocks[0], *[send(blocks[d], along_y(d)) for d in ORDER[:3]]]

    projected, square_sum = finish_sum([reduce_half(half) for half in range(2)])
    square_sum = square_sum + send(square_sum, CORE_SWAP)
    for along in (along_y, along_first, along_second):
        a, b, c = (send(square_sum, along(d)) for d in ORDER[:3])
        square_sum = (square_sum + a) + (b + c)

    *moments, update = adam(
        projected,
        square_sum,
        (avg_q, key_first_moment, value_first_moment),
        (sq_q, key_second_moment, value_second_moment),
    )

    held = jnp.concatenate([update, *[send(update, along_second(d)) for d in (1, 2, 3)]], axis=0)
    gathered = [held, *[send(held, along_first(d)) for d in (1, 2, 3)]]
    new_weights = apply_updates(
        where,
        gathered,
        projectors,
        (weight_q, key_weight_matrix, value_weight_matrix),
        (comp_q, key_compensation, value_compensation),
    )
    return (*new_weights, *moments)


def solution(mesh):
    split = Mesh(mesh.devices.reshape(4, 2, 4, 4), ALL)
    return jax.shard_map(
        shards,
        mesh=split,
        in_specs=(*[P(DP, FSDP, None)] * 3, *[P(FSDP, None)] * 3, *[P(FSDP, DP)] * 12),
        out_specs=(*[P(FSDP, DP)] * 9,),
        check_vma=False,
    )
```

```python
import math

import jax
import jax.numpy as jnp
from jax import lax
from jax.experimental import pallas as pl
from jax.experimental.pallas import tpu as pltpu
from jax.sharding import Mesh
from jax.sharding import PartitionSpec as P

QUERY_OUTPUTS = 8192
KEY_VALUE_OUTS = 1024
PROJECT_RANK = 512
STEP = 10
DP = ("dp_0", "dp_1")
FSDP = ("fsdp_0", "fsdp_1")
ALL = ("dp_0", "dp_1", "fsdp_0", "fsdp_1")

ROWS = 512
RANK_ROWS = 32
BLOCK = 128
WQ, WK = 1024, 128
WIDTH = WQ + 2 * WK
HALF = WIDTH // 2
ORDER = (1, 3, 2, 0)
SEGMENTS = (((0, 0, HALF, 0),), ((0, HALF, WQ - HALF, 0), (1, 0, WK, WQ - HALF), (2, 0, WK, WQ - HALF + WK)))


F32 = jnp.float32
BF16 = jnp.bfloat16
F16 = jnp.float16


def pairs(move):
    found = []
    for y in range(4):
        for c in range(2):
            for z in range(4):
                for x in range(4):
                    ty, tc, tz, tx = move(y, c, z, x)
                    source = ((y * 2 + c) * 4 + z) * 4 + x
                    found.append((source, ((ty * 2 + tc) * 4 + tz) * 4 + tx))
    return found


def along_first(d):
    return pairs(lambda y, c, z, x: (y, c, (z + d) % 4, x) if c == 0 else (y, c, z, (x + d) % 4))


def along_second(d):
    return pairs(lambda y, c, z, x: (y, c, z, (x + d) % 4) if c == 0 else (y, c, (z + d) % 4, x))


def along_y(d):
    return pairs(lambda y, c, z, x: ((y + d) % 4, c, z, x))


CORE_SWAP = pairs(lambda y, c, z, x: (y, 1 - c, z, x))

def send(value, route):
    return lax.ppermute(value, ALL, route)


def vmem():
    return pl.BlockSpec(memory_space=pltpu.VMEM)


def grant(mib):
    return pltpu.CompilerParams(vmem_limit_bytes=mib * 1024 * 1024)


def order_projectors(projectors):
    def body(pq_hbm, pk_hbm, pv_hbm, out_ref, pq_ref, pk_ref, pv_ref, semaphores):
        arriving = [
            pltpu.make_async_copy(source, target, semaphores.at[m])
            for m, (source, target) in enumerate(
                ((pq_hbm, pq_ref), (pk_hbm, pk_ref), (pv_hbm, pv_ref))
            )
        ]
        for copy in arriving:
            copy.start()
        for copy in arriving:
            copy.wait()
        core = lax.axis_index("dp_1")
        own = jnp.where(core == 0, lax.axis_index("fsdp_0"), lax.axis_index("fsdp_1"))
        for n, d in enumerate(ORDER):
            at = lax.broadcasted_iota(jnp.int32, (BLOCK, PROJECT_RANK), 0)
            rank = lax.broadcasted_iota(jnp.int32, (BLOCK, PROJECT_RANK), 1)
            outer, inner = at // RANK_ROWS, at % RANK_ROWS
            a = (own + d) % 4
            straight = a * BLOCK + at
            crossed = outer * BLOCK + a * RANK_ROWS + inner
            wanted = jnp.where(core == 0, straight, crossed)
            pick = jnp.where(rank == wanted, 1.0, 0.0).astype(BF16)
            for m, p_ref in enumerate((pq_ref, pk_ref, pv_ref)):
                rows = lax.dot_general(
                    pick, p_ref[...], (((1,), (1,)), ((), ())), preferred_element_type=F32
                )
                for k in range(2):
                    out_ref[m, n * BLOCK : (n + 1) * BLOCK, k * ROWS : (k + 1) * ROWS] = rows.astype(BF16)

    return pl.pallas_call(
        body,
        in_specs=[pl.BlockSpec(memory_space=pltpu.HBM)] * 3,
        out_specs=vmem(),
        out_shape=jax.ShapeDtypeStruct((3, PROJECT_RANK, 2 * ROWS), BF16),
        scratch_shapes=[
            *[pltpu.VMEM((ROWS, PROJECT_RANK), BF16)] * 3,
            pltpu.SemaphoreType.DMA((3,)),
        ],
        compiler_params=grant(12),
        name="order_projectors",
    )(*(pltpu.with_memory_space_constraint(p, pltpu.HBM) for p in projectors))


def copies(half, core, grad_refs, into, semaphores):
    blocks = []
    for y in range(4):
        block = []
        for m, low, wide, at in SEGMENTS[half]:
            start = pl.multiple_of((2 * y + core) * (WK if m else WQ) + low, 128)
            block.append(
                pltpu.make_async_copy(
                    grad_refs[m].at[:, pl.ds(start, wide)],
                    into.at[:, pl.ds(y * HALF + at, wide)],
                    semaphores.at[y * len(SEGMENTS[half]) + len(block)],
                )
            )
        blocks.append(block)
    return blocks


def take_columns(half, grads):
    parts = len(SEGMENTS[half])

    def body(q_ref, k_ref, v_ref, out_ref, held, semaphores, out_semaphores):
        other = 1 - lax.axis_index("dp_1")
        blocks = copies(half, other, (q_ref, k_ref, v_ref), held, semaphores)
        for block in blocks:
            for copy in block:
                copy.start()
        leaving = []
        for y, block in enumerate(blocks):
            for copy in block:
                copy.wait()
            span = pl.ds(y * HALF, HALF)
            copy = pltpu.make_async_copy(held.at[:, span], out_ref.at[:, span], out_semaphores.at[y])
            copy.start()
            leaving.append(copy)
        for copy in leaving:
            copy.wait()

    return pl.pallas_call(
        body,
        in_specs=[pl.BlockSpec(memory_space=pltpu.HBM)] * 3,
        out_specs=pl.BlockSpec(memory_space=pltpu.HBM),
        out_shape=jax.ShapeDtypeStruct((ROWS, 4 * HALF), BF16),
        scratch_shapes=[
            pltpu.VMEM((ROWS, 4 * HALF), BF16),
            pltpu.SemaphoreType.DMA((4 * parts,)),
            pltpu.SemaphoreType.DMA((4,)),
        ],
        compiler_params=grant(8),
        name="take_columns",
    )(*grads)


def power_of_two(peak):
    scale = jnp.full(peak.shape, 2.0**-5, F32)
    for k in range(-4, 15):
        scale = jnp.where(peak * 2.0**k <= 16384.0, 2.0**k, scale)
    return scale


def project(half, transposed, grads, received):
    parts = len(SEGMENTS[half])

    def body(t_ref, other_ref, q_ref, k_ref, v_ref, *rest):
        outs, both, semaphores, other_semaphores = rest[:4], rest[4], rest[5], rest[6]
        core = lax.axis_index("dp_1")
        blocks = copies(half, core, (q_ref, k_ref, v_ref), both.at[:ROWS], semaphores)
        for y, block in enumerate(blocks):
            span = pl.ds(y * HALF, HALF)
            block.append(
                pltpu.make_async_copy(
                    other_ref.at[:, span], both.at[pl.ds(ROWS, ROWS), span], other_semaphores.at[y]
                )
            )
            for copy in block:
                copy.start()
        largest = [jnp.zeros((8, 128), F32)] * 3
        for y, block in enumerate(blocks):
            for copy in block:
                copy.wait()
            for m, low, wide, at in SEGMENTS[half]:
                span = slice(y * HALF + at, y * HALF + at + wide)
                product = jnp.dot(t_ref[m], both[:, span], preferred_element_type=F32)
                for n in range(4):
                    piece = product[n * BLOCK : (n + 1) * BLOCK]
                    outs[n][:, span] = piece
                    if n < 3:
                        tall = jnp.abs(piece)
                        for r in range(0, BLOCK, 8):
                            for k in range(0, wide, 128):
                                largest[n] = jnp.maximum(largest[n], tall[r : r + 8, k : k + 128])
        for n in range(3):
            peak = jnp.max(jnp.max(largest[n], axis=0, keepdims=True), axis=1, keepdims=True)
            scale = power_of_two(peak)
            outs[n][:, : 4 * HALF] = outs[n][:, : 4 * HALF] * scale
            outs[n][:, 4 * HALF :] = jnp.broadcast_to(1.0 / scale, (BLOCK, 128))

    shapes = [(BLOCK, 4 * HALF + 128)] * 3 + [(BLOCK, 4 * HALF)]
    return pl.pallas_call(
        body,
        in_specs=[vmem(), pl.BlockSpec(memory_space=pl.ANY), *[pl.BlockSpec(memory_space=pltpu.HBM)] * 3],
        out_specs=[vmem()] * 4,
        out_shape=[jax.ShapeDtypeStruct(s, F32) for s in shapes],
        scratch_shapes=[
            pltpu.VMEM((2 * ROWS, 4 * HALF), BF16),
            pltpu.SemaphoreType.DMA((4 * parts,)),
            pltpu.SemaphoreType.DMA((4,)),
        ],
        compiler_params=grant(18),
        name="project",
    )(transposed, received, *grads)


def combine(half, own, arrived):
    shape = (BLOCK, HALF) if half == 0 else (RANK_ROWS, 4 * HALF)

    def body(own_ref, a_ref, b_ref, c_ref, *outs):
        core = lax.axis_index("dp_1")
        if half == 0:
            here = lax.axis_index("dp_0")
        else:
            here = jnp.where(core == 0, lax.axis_index("fsdp_1"), lax.axis_index("fsdp_0"))
        for n, d in enumerate(ORDER):
            b = (here + d) % 4
            if half == 0:
                rows = slice(0, BLOCK)
                columns = pl.ds(pl.multiple_of(b * HALF, 128), HALF)
            else:
                rows = pl.ds(pl.multiple_of(b * RANK_ROWS, RANK_ROWS), RANK_ROWS)
                columns = slice(0, 4 * HALF)
            total = own_ref[rows, columns]
            for ref in (a_ref, b_ref, c_ref):
                undo = ref[rows, 4 * HALF : 4 * HALF + 128][:, :1]
                total = total + ref[rows, columns] * undo
            outs[n][...] = total

    return pl.pallas_call(
        body,
        in_specs=[vmem()] * 4,
        out_specs=[vmem()] * 4,
        out_shape=[jax.ShapeDtypeStruct(shape, F32)] * 4,
        compiler_params=grant(14),
        name="combine",
    )(own, *(part.astype(F32) for part in arrived))


def finish_sum(halves):
    def body(*refs):
        sum_ref, square_ref = refs[8], refs[9]
        for h in range(2):
            a, b, c, d = (ref[...] for ref in refs[4 * h : 4 * h + 4])
            sum_ref[:, h * HALF : (h + 1) * HALF] = (a + b) + (c + d)
        total = sum_ref[...]
        square_ref[...] = jnp.broadcast_to(jnp.sum(total * total, keepdims=True), (8, 128))

    return pl.pallas_call(
        body,
        in_specs=[vmem()] * 8,
        out_specs=[vmem()] * 2,
        out_shape=[
            jax.ShapeDtypeStruct((RANK_ROWS, WIDTH), F32),
            jax.ShapeDtypeStruct((8, 128), F32),
        ],
        compiler_params=grant(4),
        name="finish_sum",
    )(*halves[0], *halves[1])


def adam(projected, square_sum, avgs, squares):
    threshold = math.sqrt(PROJECT_RANK * (QUERY_OUTPUTS + 2 * KEY_VALUE_OUTS))
    correct_one = 1.0 - 0.9**STEP
    correct_two = 1.0 - 0.95**STEP

    def body(p_ref, s_ref, *rest):
        avg_refs, sq_refs = rest[:3], rest[3:6]
        new_avg_refs, new_sq_refs, update_ref = rest[6:9], rest[9:12], rest[12]
        clip = jnp.minimum(1.0, threshold / jnp.sqrt(s_ref[0:1, 0:1] + 1e-06))
        at = 0
        for m in range(3):
            wide = avg_refs[m].shape[1]
            scaled = clip * p_ref[:, at : at + wide]
            new_avg = 0.9 * avg_refs[m][...] + 0.1 * scaled
            new_sq = 0.95 * sq_refs[m][...] + 0.05 * scaled * scaled
            new_avg_refs[m][...] = new_avg
            new_sq_refs[m][...] = new_sq
            update = new_avg / correct_one / (jnp.sqrt(new_sq / correct_two) + 1e-08)
            update_ref[:, at : at + wide] = update.astype(BF16)
            at += wide

    like = [jax.ShapeDtypeStruct(a.shape, F32) for a in avgs]
    return pl.pallas_call(
        body,
        out_shape=[*like, *like, jax.ShapeDtypeStruct((RANK_ROWS, WIDTH), BF16)],
        compiler_params=grant(4),
        name="adam",
    )(projected, square_sum, *avgs, *squares)


def apply_updates(gathered, projectors, weights, comps):
    tile = 128

    def body(*refs):
        parts, (pq, pk, pv), ws, cs = refs[:4], refs[4:7], refs[7:10], refs[10:13]
        outs, update, held, semaphores = refs[13:16], refs[16], refs[17:20], refs[20]

        @pl.when(pl.program_id(0) == 0)
        def _():
            arriving = [
                pltpu.make_async_copy(cs[m], held[m], semaphores.at[m]) for m in range(3)
            ]
            for copy in arriving:
                copy.start()
            core = lax.axis_index("dp_1")
            z_own, x_own = lax.axis_index("fsdp_0"), lax.axis_index("fsdp_1")
            first = jnp.where(core == 0, z_own, x_own)
            second = jnp.where(core == 0, x_own, z_own)
            for d in range(4):
                for k in range(4):
                    far = (first + 4 - d) % 4
                    near = (second + 4 - k) % 4
                    z = jnp.where(core == 0, far, near)
                    x = jnp.where(core == 0, near, far)
                    at = pl.multiple_of(z * BLOCK + x * RANK_ROWS, RANK_ROWS)
                    update[pl.ds(at, RANK_ROWS), :] = parts[d][k * RANK_ROWS : (k + 1) * RANK_ROWS, :]
            for copy in arriving:
                copy.wait()

        at = 0
        rows = pl.ds(pl.multiple_of(pl.program_id(0) * tile, tile), tile)
        for m, p_ref in enumerate((pq, pk, pv)):
            wide = ws[m].shape[1]
            product = jnp.dot(p_ref[rows, :], update[:, at : at + wide], preferred_element_type=F32)
            outs[m][...] = ws[m][rows, :].astype(F32) + (-0.04 * product + held[m][rows, :].astype(F32))
            at += wide

    def rows(i):
        return (i, 0)

    tall = [pl.BlockSpec((tile, w.shape[1]), rows) for w in weights]
    return pl.pallas_call(
        body,
        grid_spec=pltpu.PrefetchScalarGridSpec(
            num_scalar_prefetch=0,
            grid=(ROWS // tile,),
            in_specs=[*[vmem()] * 10, *[pl.BlockSpec(memory_space=pltpu.HBM)] * 3],
            out_specs=tall,
            scratch_shapes=[
                pltpu.VMEM((PROJECT_RANK, WIDTH), BF16),
                *[pltpu.VMEM(c.shape, BF16) for c in comps],
                pltpu.SemaphoreType.DMA((3,)),
            ],
        ),
        out_shape=[jax.ShapeDtypeStruct(w.shape, F32) for w in weights],
        compiler_params=grant(16),
        name="apply_updates",
    )(
        *gathered,
        *projectors,
        *weights,
        *(pltpu.with_memory_space_constraint(c, pltpu.HBM) for c in comps),
    )


def shards(
    grad_q,
    grad_k,
    grad_v,
    proj_q,
    proj_k,
    proj_v,
    weight_q,
    key_weight_matrix,
    value_weight_matrix,
    comp_q,
    key_compensation,
    value_compensation,
    avg_q,
    key_first_moment,
    value_first_moment,
    sq_q,
    key_second_moment,
    value_second_moment,
):
    grads = tuple(
        pltpu.with_memory_space_constraint(g[0], pltpu.HBM) for g in (grad_q, grad_k, grad_v)
    )
    projectors = (proj_q, proj_k, proj_v)
    y, core, z, x = (lax.axis_index(name) for name in ALL)
    second = jnp.where(core == 0, x, z)

    received = [send(take_columns(half, grads), CORE_SWAP) for half in range(2)]
    transposed = order_projectors(projectors)

    def reduce_half(half):
        *pieces, own = project(half, transposed, grads, received[half])
        arrived = [send(piece.astype(F16), along_first(d)) for d, piece in zip(ORDER, pieces)]

        def regroup(parts, cut):
            total = cut(parts[0])
            for part in parts[1:]:
                total = total + cut(part)
            return total

        if half == 0:
            *parts, kept = combine(half, own, arrived)
            parts = [kept, *[send(part, along_y(d)) for d, part in zip(ORDER, parts)]]

            def last(b):
                return regroup(
                    parts, lambda x: lax.dynamic_slice_in_dim(x, b * RANK_ROWS, RANK_ROWS, axis=0)
                )

            blocks = {d: last((second + d) % 4) for d in ORDER}
            return [blocks[0], *[send(blocks[d], along_second(d)) for d in ORDER[:3]]]

        *parts, kept = combine(half, own, arrived)
        parts = [kept, *[send(part, along_second(d)) for d, part in zip(ORDER, parts)]]

        def last(b):
            return regroup(parts, lambda x: lax.dynamic_slice_in_dim(x, b * HALF, HALF, axis=1))

        blocks = {d: last((y + d) % 4) for d in ORDER}
        return [blocks[0], *[send(blocks[d], along_y(d)) for d in ORDER[:3]]]

    projected, square_sum = finish_sum([reduce_half(half) for half in range(2)])
    square_sum = square_sum + send(square_sum, CORE_SWAP)
    for along in (along_y, along_first, along_second):
        a, b, c = (send(square_sum, along(d)) for d in ORDER[:3])
        square_sum = (square_sum + a) + (b + c)

    *moments, update = adam(
        projected,
        square_sum,
        (avg_q, key_first_moment, value_first_moment),
        (sq_q, key_second_moment, value_second_moment),
    )

    held = jnp.concatenate([update, *[send(update, along_second(d)) for d in (1, 2, 3)]], axis=0)
    gathered = [held, *[send(held, along_first(d)) for d in (1, 2, 3)]]
    new_weights = apply_updates(
        gathered,
        projectors,
        (weight_q, key_weight_matrix, value_weight_matrix),
        (comp_q, key_compensation, value_compensation),
    )
    return (*new_weights, *moments)


def solution(mesh):
    split = Mesh(mesh.devices.reshape(4, 2, 4, 4), ALL)
    return jax.shard_map(
        shards,
        mesh=split,
        in_specs=(*[P(DP, FSDP, None)] * 3, *[P(FSDP, None)] * 3, *[P(FSDP, DP)] * 12),
        out_specs=(*[P(FSDP, DP)] * 9,),
        check_vma=False,
    )
```

```python
import math

import jax
import jax.numpy as jnp
from jax import lax
from jax.experimental import pallas as pl
from jax.experimental.pallas import tpu as pltpu
from jax.sharding import Mesh
from jax.sharding import PartitionSpec as P

QUERY_OUTPUTS = 8192
KEY_VALUE_OUTS = 1024
PROJECT_RANK = 512
STEP = 10
DP = ("dp_0", "dp_1")
FSDP = ("fsdp_0", "fsdp_1")
ALL = ("dp_0", "dp_1", "fsdp_0", "fsdp_1")

ROWS = 512
RANK_ROWS = 32
BLOCK = 128
WQ, WK = 1024, 128
WIDTH = WQ + 2 * WK
HALF = WIDTH // 2
ORDER = (1, 3, 2, 0)
SEGMENTS = (((0, 0, HALF, 0),), ((0, HALF, WQ - HALF, 0), (1, 0, WK, WQ - HALF), (2, 0, WK, WQ - HALF + WK)))


F32 = jnp.float32
BF16 = jnp.bfloat16
F16 = jnp.float16


def pairs(move):
    found = []
    for y in range(4):
        for c in range(2):
            for z in range(4):
                for x in range(4):
                    ty, tc, tz, tx = move(y, c, z, x)
                    source = ((y * 2 + c) * 4 + z) * 4 + x
                    found.append((source, ((ty * 2 + tc) * 4 + tz) * 4 + tx))
    return found


def along_first(d):
    return pairs(lambda y, c, z, x: (y, c, (z + d) % 4, x) if c == 0 else (y, c, z, (x + d) % 4))


def along_second(d):
    return pairs(lambda y, c, z, x: (y, c, z, (x + d) % 4) if c == 0 else (y, c, (z + d) % 4, x))


def along_y(d):
    return pairs(lambda y, c, z, x: ((y + d) % 4, c, z, x))


CORE_SWAP = pairs(lambda y, c, z, x: (y, 1 - c, z, x))

def send(value, route):
    return lax.ppermute(value, ALL, route)


def vmem():
    return pl.BlockSpec(memory_space=pltpu.VMEM)


def grant(mib):
    return pltpu.CompilerParams(vmem_limit_bytes=mib * 1024 * 1024)


def order_projectors(projectors):
    def body(pq_hbm, pk_hbm, pv_hbm, out_ref, pq_ref, pk_ref, pv_ref, semaphores):
        arriving = [
            pltpu.make_async_copy(source, target, semaphores.at[m])
            for m, (source, target) in enumerate(
                ((pq_hbm, pq_ref), (pk_hbm, pk_ref), (pv_hbm, pv_ref))
            )
        ]
        for copy in arriving:
            copy.start()
        for copy in arriving:
            copy.wait()
        core = lax.axis_index("dp_1")
        own = jnp.where(core == 0, lax.axis_index("fsdp_0"), lax.axis_index("fsdp_1"))
        for n, d in enumerate(ORDER):
            at = lax.broadcasted_iota(jnp.int32, (BLOCK, PROJECT_RANK), 0)
            rank = lax.broadcasted_iota(jnp.int32, (BLOCK, PROJECT_RANK), 1)
            outer, inner = at // RANK_ROWS, at % RANK_ROWS
            a = (own + d) % 4
            straight = a * BLOCK + at
            crossed = outer * BLOCK + a * RANK_ROWS + inner
            wanted = jnp.where(core == 0, straight, crossed)
            pick = jnp.where(rank == wanted, 1.0, 0.0).astype(BF16)
            for m, p_ref in enumerate((pq_ref, pk_ref, pv_ref)):
                rows = lax.dot_general(
                    pick, p_ref[...], (((1,), (1,)), ((), ())), preferred_element_type=F32
                )
                for k in range(2):
                    out_ref[m, n * BLOCK : (n + 1) * BLOCK, k * ROWS : (k + 1) * ROWS] = rows.astype(BF16)

    return pl.pallas_call(
        body,
        in_specs=[pl.BlockSpec(memory_space=pltpu.HBM)] * 3,
        out_specs=vmem(),
        out_shape=jax.ShapeDtypeStruct((3, PROJECT_RANK, 2 * ROWS), BF16),
        scratch_shapes=[
            *[pltpu.VMEM((ROWS, PROJECT_RANK), BF16)] * 3,
            pltpu.SemaphoreType.DMA((3,)),
        ],
        compiler_params=grant(12),
        name="order_projectors",
    )(*(pltpu.with_memory_space_constraint(p, pltpu.HBM) for p in projectors))


def copies(half, core, grad_refs, into, semaphores):
    blocks = []
    for y in range(4):
        block = []
        for m, low, wide, at in SEGMENTS[half]:
            start = pl.multiple_of((2 * y + core) * (WK if m else WQ) + low, 128)
            block.append(
                pltpu.make_async_copy(
                    grad_refs[m].at[:, pl.ds(start, wide)],
                    into.at[:, pl.ds(y * HALF + at, wide)],
                    semaphores.at[y * len(SEGMENTS[half]) + len(block)],
                )
            )
        blocks.append(block)
    return blocks


def take_columns(half, grads):
    parts = len(SEGMENTS[half])

    def body(q_ref, k_ref, v_ref, out_ref, held, semaphores, out_semaphores):
        other = 1 - lax.axis_index("dp_1")
        blocks = copies(half, other, (q_ref, k_ref, v_ref), held, semaphores)
        for block in blocks:
            for copy in block:
                copy.start()
        leaving = []
        for y, block in enumerate(blocks):
            for copy in block:
                copy.wait()
            span = pl.ds(y * HALF, HALF)
            copy = pltpu.make_async_copy(held.at[:, span], out_ref.at[:, span], out_semaphores.at[y])
            copy.start()
            leaving.append(copy)
        for copy in leaving:
            copy.wait()

    return pl.pallas_call(
        body,
        in_specs=[pl.BlockSpec(memory_space=pltpu.HBM)] * 3,
        out_specs=pl.BlockSpec(memory_space=pltpu.HBM),
        out_shape=jax.ShapeDtypeStruct((ROWS, 4 * HALF), BF16),
        scratch_shapes=[
            pltpu.VMEM((ROWS, 4 * HALF), BF16),
            pltpu.SemaphoreType.DMA((4 * parts,)),
            pltpu.SemaphoreType.DMA((4,)),
        ],
        compiler_params=grant(8),
        name="take_columns",
    )(*grads)


def power_of_two(peak):
    scale = jnp.full(peak.shape, 2.0**-5, F32)
    for k in range(-4, 15):
        scale = jnp.where(peak * 2.0**k <= 16384.0, 2.0**k, scale)
    return scale


def project(half, transposed, grads, received):
    parts = len(SEGMENTS[half])

    def body(t_ref, other_ref, q_ref, k_ref, v_ref, *rest):
        outs, both, semaphores, other_semaphores = rest[:4], rest[4], rest[5], rest[6]
        core = lax.axis_index("dp_1")
        arriving, base = {}, {}
        for k, (m, low, wide, at) in enumerate(SEGMENTS[half]):
            base[m] = 4 * at
            for y in range(4):
                start = pl.multiple_of((2 * y + core) * (WK if m else WQ) + low, 128)
                span = pl.ds(base[m] + y * wide, wide)
                arriving[m, y] = (
                    pltpu.make_async_copy(
                        (q_ref, k_ref, v_ref)[m].at[:, pl.ds(start, wide)],
                        both.at[pl.ds(0, ROWS), span],
                        semaphores.at[y * parts + k],
                    ),
                    pltpu.make_async_copy(
                        other_ref.at[:, pl.ds(y * HALF + at, wide)],
                        both.at[pl.ds(ROWS, ROWS), span],
                        other_semaphores.at[y * parts + k],
                    ),
                )
                for copy in arriving[m, y]:
                    copy.start()
        largest = [jnp.zeros((8, 128), F32)] * 3
        for m, low, wide, at in SEGMENTS[half]:
            for group in ((0, 1), (2, 3)) if m == 0 else ((0, 1, 2, 3),):
                for y in group:
                    for copy in arriving[m, y]:
                        copy.wait()
                first = base[m] + group[0] * wide
                columns = both[:, first : first + len(group) * wide]
                product = jnp.dot(t_ref[m], columns, preferred_element_type=F32)
                for n in range(4):
                    for k, y in enumerate(group):
                        piece = product[n * BLOCK : (n + 1) * BLOCK, k * wide : (k + 1) * wide]
                        outs[n][:, y * HALF + at : y * HALF + at + wide] = piece
                        if n < 3:
                            tall = jnp.abs(piece)
                            for r in range(0, BLOCK, 8):
                                for c in range(0, wide, 128):
                                    largest[n] = jnp.maximum(largest[n], tall[r : r + 8, c : c + 128])
        for n in range(3):
            peak = jnp.max(jnp.max(largest[n], axis=0, keepdims=True), axis=1, keepdims=True)
            scale = power_of_two(peak)
            outs[n][:, : 4 * HALF] = outs[n][:, : 4 * HALF] * scale
            outs[n][:, 4 * HALF :] = jnp.broadcast_to(1.0 / scale, (BLOCK, 128))

    shapes = [(BLOCK, 4 * HALF + 128)] * 3 + [(BLOCK, 4 * HALF)]
    return pl.pallas_call(
        body,
        in_specs=[vmem(), pl.BlockSpec(memory_space=pl.ANY), *[pl.BlockSpec(memory_space=pltpu.HBM)] * 3],
        out_specs=[vmem()] * 4,
        out_shape=[jax.ShapeDtypeStruct(s, F32) for s in shapes],
        scratch_shapes=[
            pltpu.VMEM((2 * ROWS, 4 * HALF), BF16),
            pltpu.SemaphoreType.DMA((4 * parts,)),
            pltpu.SemaphoreType.DMA((4 * parts,)),
        ],
        compiler_params=grant(18),
        name="project",
    )(transposed, received, *grads)


def combine(half, own, arrived):
    shape = (BLOCK, HALF) if half == 0 else (RANK_ROWS, 4 * HALF)

    def body(own_ref, a_ref, b_ref, c_ref, *outs):
        core = lax.axis_index("dp_1")
        if half == 0:
            here = lax.axis_index("dp_0")
        else:
            here = jnp.where(core == 0, lax.axis_index("fsdp_1"), lax.axis_index("fsdp_0"))
        for n, d in enumerate(ORDER):
            b = (here + d) % 4
            if half == 0:
                rows = slice(0, BLOCK)
                columns = pl.ds(pl.multiple_of(b * HALF, 128), HALF)
            else:
                rows = pl.ds(pl.multiple_of(b * RANK_ROWS, RANK_ROWS), RANK_ROWS)
                columns = slice(0, 4 * HALF)
            total = own_ref[rows, columns]
            for ref in (a_ref, b_ref, c_ref):
                undo = ref[rows, 4 * HALF : 4 * HALF + 128][:, :1]
                total = total + ref[rows, columns] * undo
            outs[n][...] = total

    return pl.pallas_call(
        body,
        in_specs=[vmem()] * 4,
        out_specs=[vmem()] * 4,
        out_shape=[jax.ShapeDtypeStruct(shape, F32)] * 4,
        compiler_params=grant(14),
        name="combine",
    )(own, *(part.astype(F32) for part in arrived))


def finish_sum(halves):
    def body(*refs):
        sum_ref, square_ref = refs[8], refs[9]
        for h in range(2):
            a, b, c, d = (ref[...] for ref in refs[4 * h : 4 * h + 4])
            sum_ref[:, h * HALF : (h + 1) * HALF] = (a + b) + (c + d)
        total = sum_ref[...]
        square_ref[...] = jnp.broadcast_to(jnp.sum(total * total, keepdims=True), (8, 128))

    return pl.pallas_call(
        body,
        in_specs=[vmem()] * 8,
        out_specs=[vmem()] * 2,
        out_shape=[
            jax.ShapeDtypeStruct((RANK_ROWS, WIDTH), F32),
            jax.ShapeDtypeStruct((8, 128), F32),
        ],
        compiler_params=grant(4),
        name="finish_sum",
    )(*halves[0], *halves[1])


def adam(projected, square_sum, avgs, squares):
    threshold = math.sqrt(PROJECT_RANK * (QUERY_OUTPUTS + 2 * KEY_VALUE_OUTS))
    correct_one = 1.0 - 0.9**STEP
    correct_two = 1.0 - 0.95**STEP

    def body(p_ref, s_ref, *rest):
        avg_refs, sq_refs = rest[:3], rest[3:6]
        new_avg_refs, new_sq_refs, update_ref = rest[6:9], rest[9:12], rest[12]
        clip = jnp.minimum(1.0, threshold / jnp.sqrt(s_ref[0:1, 0:1] + 1e-06))
        at = 0
        for m in range(3):
            wide = avg_refs[m].shape[1]
            scaled = clip * p_ref[:, at : at + wide]
            new_avg = 0.9 * avg_refs[m][...] + 0.1 * scaled
            new_sq = 0.95 * sq_refs[m][...] + 0.05 * scaled * scaled
            new_avg_refs[m][...] = new_avg
            new_sq_refs[m][...] = new_sq
            update = new_avg / correct_one / (jnp.sqrt(new_sq / correct_two) + 1e-08)
            update_ref[:, at : at + wide] = update.astype(BF16)
            at += wide

    like = [jax.ShapeDtypeStruct(a.shape, F32) for a in avgs]
    return pl.pallas_call(
        body,
        out_shape=[*like, *like, jax.ShapeDtypeStruct((RANK_ROWS, WIDTH), BF16)],
        compiler_params=grant(4),
        name="adam",
    )(projected, square_sum, *avgs, *squares)


def apply_updates(gathered, projectors, weights, comps):
    tile = 128

    def body(*refs):
        parts, (pq, pk, pv), ws, cs = refs[:4], refs[4:7], refs[7:10], refs[10:13]
        outs, update, held, semaphores = refs[13:16], refs[16], refs[17:20], refs[20]

        @pl.when(pl.program_id(0) == 0)
        def _():
            arriving = [
                pltpu.make_async_copy(cs[m], held[m], semaphores.at[m]) for m in range(3)
            ]
            for copy in arriving:
                copy.start()
            core = lax.axis_index("dp_1")
            z_own, x_own = lax.axis_index("fsdp_0"), lax.axis_index("fsdp_1")
            first = jnp.where(core == 0, z_own, x_own)
            second = jnp.where(core == 0, x_own, z_own)
            for d in range(4):
                for k in range(4):
                    far = (first + 4 - d) % 4
                    near = (second + 4 - k) % 4
                    z = jnp.where(core == 0, far, near)
                    x = jnp.where(core == 0, near, far)
                    at = pl.multiple_of(z * BLOCK + x * RANK_ROWS, RANK_ROWS)
                    update[pl.ds(at, RANK_ROWS), :] = parts[d][k * RANK_ROWS : (k + 1) * RANK_ROWS, :]
            for copy in arriving:
                copy.wait()

        at = 0
        rows = pl.ds(pl.multiple_of(pl.program_id(0) * tile, tile), tile)
        for m, p_ref in enumerate((pq, pk, pv)):
            wide = ws[m].shape[1]
            product = jnp.dot(p_ref[rows, :], update[:, at : at + wide], preferred_element_type=F32)
            outs[m][...] = ws[m][rows, :].astype(F32) + (-0.04 * product + held[m][rows, :].astype(F32))
            at += wide

    def rows(i):
        return (i, 0)

    tall = [pl.BlockSpec((tile, w.shape[1]), rows) for w in weights]
    return pl.pallas_call(
        body,
        grid_spec=pltpu.PrefetchScalarGridSpec(
            num_scalar_prefetch=0,
            grid=(ROWS // tile,),
            in_specs=[*[vmem()] * 10, *[pl.BlockSpec(memory_space=pltpu.HBM)] * 3],
            out_specs=tall,
            scratch_shapes=[
                pltpu.VMEM((PROJECT_RANK, WIDTH), BF16),
                *[pltpu.VMEM(c.shape, BF16) for c in comps],
                pltpu.SemaphoreType.DMA((3,)),
            ],
        ),
        out_shape=[jax.ShapeDtypeStruct(w.shape, F32) for w in weights],
        compiler_params=grant(16),
        name="apply_updates",
    )(
        *gathered,
        *projectors,
        *weights,
        *(pltpu.with_memory_space_constraint(c, pltpu.HBM) for c in comps),
    )


def shards(
    grad_q,
    grad_k,
    grad_v,
    proj_q,
    proj_k,
    proj_v,
    weight_q,
    key_weight_matrix,
    value_weight_matrix,
    comp_q,
    key_compensation,
    value_compensation,
    avg_q,
    key_first_moment,
    value_first_moment,
    sq_q,
    key_second_moment,
    value_second_moment,
):
    grads = tuple(
        pltpu.with_memory_space_constraint(g[0], pltpu.HBM) for g in (grad_q, grad_k, grad_v)
    )
    projectors = (proj_q, proj_k, proj_v)
    y, core, z, x = (lax.axis_index(name) for name in ALL)
    second = jnp.where(core == 0, x, z)

    received = [send(take_columns(half, grads), CORE_SWAP) for half in range(2)]
    transposed = order_projectors(projectors)

    def reduce_half(half):
        *pieces, own = project(half, transposed, grads, received[half])
        arrived = [send(piece.astype(F16), along_first(d)) for d, piece in zip(ORDER, pieces)]

        def regroup(parts, cut):
            total = cut(parts[0])
            for part in parts[1:]:
                total = total + cut(part)
            return total

        if half == 0:
            *parts, kept = combine(half, own, arrived)
            parts = [kept, *[send(part, along_y(d)) for d, part in zip(ORDER, parts)]]

            def last(b):
                return regroup(
                    parts, lambda x: lax.dynamic_slice_in_dim(x, b * RANK_ROWS, RANK_ROWS, axis=0)
                )

            blocks = {d: last((second + d) % 4) for d in ORDER}
            return [blocks[0], *[send(blocks[d], along_second(d)) for d in ORDER[:3]]]

        *parts, kept = combine(half, own, arrived)
        parts = [kept, *[send(part, along_second(d)) for d, part in zip(ORDER, parts)]]

        def last(b):
            return regroup(parts, lambda x: lax.dynamic_slice_in_dim(x, b * HALF, HALF, axis=1))

        blocks = {d: last((y + d) % 4) for d in ORDER}
        return [blocks[0], *[send(blocks[d], along_y(d)) for d in ORDER[:3]]]

    projected, square_sum = finish_sum([reduce_half(half) for half in range(2)])
    square_sum = square_sum + send(square_sum, CORE_SWAP)
    for along in (along_y, along_first, along_second):
        a, b, c = (send(square_sum, along(d)) for d in ORDER[:3])
        square_sum = (square_sum + a) + (b + c)

    *moments, update = adam(
        projected,
        square_sum,
        (avg_q, key_first_moment, value_first_moment),
        (sq_q, key_second_moment, value_second_moment),
    )

    held = jnp.concatenate([update, *[send(update, along_second(d)) for d in (1, 2, 3)]], axis=0)
    gathered = [held, *[send(held, along_first(d)) for d in (1, 2, 3)]]
    new_weights = apply_updates(
        gathered,
        projectors,
        (weight_q, key_weight_matrix, value_weight_matrix),
        (comp_q, key_compensation, value_compensation),
    )
    return (*new_weights, *moments)


def solution(mesh):
    split = Mesh(mesh.devices.reshape(4, 2, 4, 4), ALL)
    return jax.shard_map(
        shards,
        mesh=split,
        in_specs=(*[P(DP, FSDP, None)] * 3, *[P(FSDP, None)] * 3, *[P(FSDP, DP)] * 12),
        out_specs=(*[P(FSDP, DP)] * 9,),
        check_vma=False,
    )
```

```python
import math

import jax
import jax.numpy as jnp
from jax import lax
from jax.experimental import pallas as pl
from jax.experimental.pallas import tpu as pltpu
from jax.sharding import Mesh
from jax.sharding import PartitionSpec as P

QUERY_OUTPUTS = 8192
KEY_VALUE_OUTS = 1024
PROJECT_RANK = 512
STEP = 10
DP = ("dp_0", "dp_1")
FSDP = ("fsdp_0", "fsdp_1")
ALL = ("dp_0", "dp_1", "fsdp_0", "fsdp_1")

ROWS = 512
RANK_ROWS = 32
BLOCK = 128
WQ, WK = 1024, 128
WIDTH = WQ + 2 * WK
HALF = WIDTH // 2
ORDER = (1, 3, 2, 0)
SEGMENTS = (((0, 0, HALF, 0),), ((0, HALF, WQ - HALF, 0), (1, 0, WK, WQ - HALF), (2, 0, WK, WQ - HALF + WK)))


F32 = jnp.float32
BF16 = jnp.bfloat16
F16 = jnp.float16


def pairs(move):
    found = []
    for y in range(4):
        for c in range(2):
            for z in range(4):
                for x in range(4):
                    ty, tc, tz, tx = move(y, c, z, x)
                    source = ((y * 2 + c) * 4 + z) * 4 + x
                    found.append((source, ((ty * 2 + tc) * 4 + tz) * 4 + tx))
    return found


def along_first(d):
    return pairs(lambda y, c, z, x: (y, c, (z + d) % 4, x) if c == 0 else (y, c, z, (x + d) % 4))


def along_second(d):
    return pairs(lambda y, c, z, x: (y, c, z, (x + d) % 4) if c == 0 else (y, c, (z + d) % 4, x))


def along_y(d):
    return pairs(lambda y, c, z, x: ((y + d) % 4, c, z, x))


CORE_SWAP = pairs(lambda y, c, z, x: (y, 1 - c, z, x))

def send(value, route):
    return lax.ppermute(value, ALL, route)


def vmem():
    return pl.BlockSpec(memory_space=pltpu.VMEM)


def grant(mib):
    return pltpu.CompilerParams(vmem_limit_bytes=mib * 1024 * 1024)


def order_projectors(projectors):
    def body(pq_hbm, pk_hbm, pv_hbm, out_ref, pq_ref, pk_ref, pv_ref, semaphores):
        arriving = [
            pltpu.make_async_copy(source, target, semaphores.at[m])
            for m, (source, target) in enumerate(
                ((pq_hbm, pq_ref), (pk_hbm, pk_ref), (pv_hbm, pv_ref))
            )
        ]
        for copy in arriving:
            copy.start()
        for copy in arriving:
            copy.wait()
        core = lax.axis_index("dp_1")
        own = jnp.where(core == 0, lax.axis_index("fsdp_0"), lax.axis_index("fsdp_1"))
        for n, d in enumerate(ORDER):
            at = lax.broadcasted_iota(jnp.int32, (BLOCK, PROJECT_RANK), 0)
            rank = lax.broadcasted_iota(jnp.int32, (BLOCK, PROJECT_RANK), 1)
            outer, inner = at // RANK_ROWS, at % RANK_ROWS
            a = (own + d) % 4
            straight = a * BLOCK + at
            crossed = outer * BLOCK + a * RANK_ROWS + inner
            wanted = jnp.where(core == 0, straight, crossed)
            pick = jnp.where(rank == wanted, 1.0, 0.0).astype(BF16)
            for m, p_ref in enumerate((pq_ref, pk_ref, pv_ref)):
                rows = lax.dot_general(
                    pick, p_ref[...], (((1,), (1,)), ((), ())), preferred_element_type=F32
                )
                for k in range(2):
                    out_ref[m, n * BLOCK : (n + 1) * BLOCK, k * ROWS : (k + 1) * ROWS] = rows.astype(BF16)

    return pl.pallas_call(
        body,
        in_specs=[pl.BlockSpec(memory_space=pltpu.HBM)] * 3,
        out_specs=vmem(),
        out_shape=jax.ShapeDtypeStruct((3, PROJECT_RANK, 2 * ROWS), BF16),
        scratch_shapes=[
            *[pltpu.VMEM((ROWS, PROJECT_RANK), BF16)] * 3,
            pltpu.SemaphoreType.DMA((3,)),
        ],
        compiler_params=grant(12),
        name="order_projectors",
    )(*(pltpu.with_memory_space_constraint(p, pltpu.HBM) for p in projectors))


def copies(half, core, grad_refs, into, semaphores):
    blocks = []
    for y in range(4):
        block = []
        for m, low, wide, at in SEGMENTS[half]:
            start = pl.multiple_of((2 * y + core) * (WK if m else WQ) + low, 128)
            block.append(
                pltpu.make_async_copy(
                    grad_refs[m].at[:, pl.ds(start, wide)],
                    into.at[:, pl.ds(y * HALF + at, wide)],
                    semaphores.at[y * len(SEGMENTS[half]) + len(block)],
                )
            )
        blocks.append(block)
    return blocks


def take_columns(half, grads):
    parts = len(SEGMENTS[half])

    def body(q_ref, k_ref, v_ref, out_ref, held, semaphores, out_semaphores):
        other = 1 - lax.axis_index("dp_1")
        blocks = copies(half, other, (q_ref, k_ref, v_ref), held, semaphores)
        for block in blocks:
            for copy in block:
                copy.start()
        leaving = []
        for y, block in enumerate(blocks):
            for copy in block:
                copy.wait()
            span = pl.ds(y * HALF, HALF)
            copy = pltpu.make_async_copy(held.at[:, span], out_ref.at[:, span], out_semaphores.at[y])
            copy.start()
            leaving.append(copy)
        for copy in leaving:
            copy.wait()

    return pl.pallas_call(
        body,
        in_specs=[pl.BlockSpec(memory_space=pltpu.HBM)] * 3,
        out_specs=pl.BlockSpec(memory_space=pltpu.HBM),
        out_shape=jax.ShapeDtypeStruct((ROWS, 4 * HALF), BF16),
        scratch_shapes=[
            pltpu.VMEM((ROWS, 4 * HALF), BF16),
            pltpu.SemaphoreType.DMA((4 * parts,)),
            pltpu.SemaphoreType.DMA((4,)),
        ],
        compiler_params=grant(8),
        name="take_columns",
    )(*grads)


def power_of_two(peak):
    scale = jnp.full(peak.shape, 2.0**-5, F32)
    for k in range(-4, 15):
        scale = jnp.where(peak * 2.0**k <= 16384.0, 2.0**k, scale)
    return scale


def project(half, transposed, grads, received):
    parts = len(SEGMENTS[half])

    def body(t_ref, other_ref, q_ref, k_ref, v_ref, *rest):
        outs, both, semaphores, other_semaphores = rest[:4], rest[4], rest[5], rest[6]
        core = lax.axis_index("dp_1")
        arriving, base = {}, {}
        for k, (m, low, wide, at) in enumerate(SEGMENTS[half]):
            base[m] = 4 * at
            for y in range(4):
                start = pl.multiple_of((2 * y + core) * (WK if m else WQ) + low, 128)
                span = pl.ds(base[m] + y * wide, wide)
                arriving[m, y] = (
                    pltpu.make_async_copy(
                        (q_ref, k_ref, v_ref)[m].at[:, pl.ds(start, wide)],
                        both.at[pl.ds(0, ROWS), span],
                        semaphores.at[y * parts + k],
                    ),
                    pltpu.make_async_copy(
                        other_ref.at[:, pl.ds(y * HALF + at, wide)],
                        both.at[pl.ds(ROWS, ROWS), span],
                        other_semaphores.at[y * parts + k],
                    ),
                )
                for copy in arriving[m, y]:
                    copy.start()
        largest = [jnp.zeros((8, 128), F32)] * 3
        for m, low, wide, at in SEGMENTS[half]:
            for group in ((0, 1), (2, 3)) if m == 0 else ((0, 1, 2, 3),):
                for y in group:
                    for copy in arriving[m, y]:
                        copy.wait()
                first = base[m] + group[0] * wide
                columns = both[:, first : first + len(group) * wide]
                product = jnp.dot(t_ref[m], columns, preferred_element_type=F32)
                for n in range(4):
                    for k, y in enumerate(group):
                        piece = product[n * BLOCK : (n + 1) * BLOCK, k * wide : (k + 1) * wide]
                        outs[n][:, y * HALF + at : y * HALF + at + wide] = piece
                        if n < 3:
                            tall = jnp.abs(piece)
                            for r in range(0, BLOCK, 8):
                                for c in range(0, wide, 128):
                                    largest[n] = jnp.maximum(largest[n], tall[r : r + 8, c : c + 128])
        for n in range(3):
            peak = jnp.max(jnp.max(largest[n], axis=0, keepdims=True), axis=1, keepdims=True)
            scale = power_of_two(peak)
            outs[n][:, : 4 * HALF] = outs[n][:, : 4 * HALF] * scale
            outs[n][:, 4 * HALF :] = jnp.broadcast_to(1.0 / scale, (BLOCK, 128))

    shapes = [(BLOCK, 4 * HALF + 128)] * 3 + [(BLOCK, 4 * HALF)]
    return pl.pallas_call(
        body,
        in_specs=[vmem(), pl.BlockSpec(memory_space=pl.ANY), *[pl.BlockSpec(memory_space=pltpu.HBM)] * 3],
        out_specs=[vmem()] * 4,
        out_shape=[jax.ShapeDtypeStruct(s, F32) for s in shapes],
        scratch_shapes=[
            pltpu.VMEM((2 * ROWS, 4 * HALF), BF16),
            pltpu.SemaphoreType.DMA((4 * parts,)),
            pltpu.SemaphoreType.DMA((4 * parts,)),
        ],
        compiler_params=grant(18),
        name="project",
    )(transposed, received, *grads)


def combine(half, own, arrived):
    shape = (BLOCK, HALF) if half == 0 else (RANK_ROWS, 4 * HALF)

    def body(own_ref, a_ref, b_ref, c_ref, *outs):
        core = lax.axis_index("dp_1")
        if half == 0:
            here = lax.axis_index("dp_0")
        else:
            here = jnp.where(core == 0, lax.axis_index("fsdp_1"), lax.axis_index("fsdp_0"))
        for n, d in enumerate(ORDER):
            b = (here + d) % 4
            if half == 0:
                rows = slice(0, BLOCK)
                columns = pl.ds(pl.multiple_of(b * HALF, 128), HALF)
            else:
                rows = pl.ds(pl.multiple_of(b * RANK_ROWS, RANK_ROWS), RANK_ROWS)
                columns = slice(0, 4 * HALF)
            total = own_ref[rows, columns]
            for ref in (a_ref, b_ref, c_ref):
                undo = ref[rows, 4 * HALF : 4 * HALF + 128][:, :1]
                total = total + ref[rows, columns] * undo
            outs[n][...] = total

    return pl.pallas_call(
        body,
        in_specs=[vmem()] * 4,
        out_specs=[vmem()] * 4,
        out_shape=[jax.ShapeDtypeStruct(shape, F32)] * 4,
        compiler_params=grant(14),
        name="combine",
    )(own, *(part.astype(F32) for part in arrived))


def finish_sum(halves):
    def body(*refs):
        sum_ref, square_ref = refs[8], refs[9]
        for h in range(2):
            a, b, c, d = (ref[...] for ref in refs[4 * h : 4 * h + 4])
            sum_ref[:, h * HALF : (h + 1) * HALF] = (a + b) + (c + d)
        total = sum_ref[...]
        square_ref[...] = jnp.broadcast_to(jnp.sum(total * total, keepdims=True), (8, 128))

    return pl.pallas_call(
        body,
        in_specs=[vmem()] * 8,
        out_specs=[vmem()] * 2,
        out_shape=[
            jax.ShapeDtypeStruct((RANK_ROWS, WIDTH), F32),
            jax.ShapeDtypeStruct((8, 128), F32),
        ],
        compiler_params=grant(4),
        name="finish_sum",
    )(*halves[0], *halves[1])


def adam(projected, square_sum, avgs, squares):
    threshold = math.sqrt(PROJECT_RANK * (QUERY_OUTPUTS + 2 * KEY_VALUE_OUTS))
    correct_one = 1.0 - 0.9**STEP
    correct_two = 1.0 - 0.95**STEP

    def body(p_ref, s_ref, *rest):
        avg_refs, sq_refs = rest[:3], rest[3:6]
        new_avg_refs, new_sq_refs, update_ref = rest[6:9], rest[9:12], rest[12]
        clip = jnp.minimum(1.0, threshold / jnp.sqrt(s_ref[0:1, 0:1] + 1e-06))
        at = 0
        for m in range(3):
            wide = avg_refs[m].shape[1]
            scaled = clip * p_ref[:, at : at + wide]
            new_avg = 0.9 * avg_refs[m][...] + 0.1 * scaled
            new_sq = 0.95 * sq_refs[m][...] + 0.05 * scaled * scaled
            new_avg_refs[m][...] = new_avg
            new_sq_refs[m][...] = new_sq
            update = new_avg / correct_one / (jnp.sqrt(new_sq / correct_two) + 1e-08)
            update_ref[:, at : at + wide] = update.astype(BF16)
            at += wide

    like = [jax.ShapeDtypeStruct(a.shape, F32) for a in avgs]
    return pl.pallas_call(
        body,
        out_shape=[*like, *like, jax.ShapeDtypeStruct((RANK_ROWS, WIDTH), BF16)],
        compiler_params=grant(4),
        name="adam",
    )(projected, square_sum, *avgs, *squares)


def apply_updates(gathered, projectors, weights, comps):
    tile = 256

    def body(*refs):
        parts, (pq, pk, pv), ws, cs = refs[:4], refs[4:7], refs[7:10], refs[10:13]
        outs, update, held, semaphores = refs[13:16], refs[16], refs[17:20], refs[20]

        @pl.when(pl.program_id(0) == 0)
        def _():
            arriving = [
                pltpu.make_async_copy(cs[m], held[m], semaphores.at[m]) for m in range(3)
            ]
            for copy in arriving:
                copy.start()
            core = lax.axis_index("dp_1")
            z_own, x_own = lax.axis_index("fsdp_0"), lax.axis_index("fsdp_1")
            first = jnp.where(core == 0, z_own, x_own)
            second = jnp.where(core == 0, x_own, z_own)
            for d in range(4):
                for k in range(4):
                    far = (first + 4 - d) % 4
                    near = (second + 4 - k) % 4
                    z = jnp.where(core == 0, far, near)
                    x = jnp.where(core == 0, near, far)
                    at = pl.multiple_of(z * BLOCK + x * RANK_ROWS, RANK_ROWS)
                    update[pl.ds(at, RANK_ROWS), :] = parts[d][k * RANK_ROWS : (k + 1) * RANK_ROWS, :]
            for copy in arriving:
                copy.wait()

        at = 0
        rows = pl.ds(pl.multiple_of(pl.program_id(0) * tile, tile), tile)
        for m, p_ref in enumerate((pq, pk, pv)):
            wide = ws[m].shape[1]
            product = jnp.dot(p_ref[rows, :], update[:, at : at + wide], preferred_element_type=F32)
            outs[m][...] = ws[m][rows, :].astype(F32) + (-0.04 * product + held[m][rows, :].astype(F32))
            at += wide

    def rows(i):
        return (i, 0)

    tall = [pl.BlockSpec((tile, w.shape[1]), rows) for w in weights]
    return pl.pallas_call(
        body,
        grid_spec=pltpu.PrefetchScalarGridSpec(
            num_scalar_prefetch=0,
            grid=(ROWS // tile,),
            in_specs=[*[vmem()] * 10, *[pl.BlockSpec(memory_space=pltpu.HBM)] * 3],
            out_specs=tall,
            scratch_shapes=[
                pltpu.VMEM((PROJECT_RANK, WIDTH), BF16),
                *[pltpu.VMEM(c.shape, BF16) for c in comps],
                pltpu.SemaphoreType.DMA((3,)),
            ],
        ),
        out_shape=[jax.ShapeDtypeStruct(w.shape, F32) for w in weights],
        compiler_params=grant(16),
        name="apply_updates",
    )(
        *gathered,
        *projectors,
        *weights,
        *(pltpu.with_memory_space_constraint(c, pltpu.HBM) for c in comps),
    )


def shards(
    grad_q,
    grad_k,
    grad_v,
    proj_q,
    proj_k,
    proj_v,
    weight_q,
    key_weight_matrix,
    value_weight_matrix,
    comp_q,
    key_compensation,
    value_compensation,
    avg_q,
    key_first_moment,
    value_first_moment,
    sq_q,
    key_second_moment,
    value_second_moment,
):
    grads = tuple(
        pltpu.with_memory_space_constraint(g[0], pltpu.HBM) for g in (grad_q, grad_k, grad_v)
    )
    projectors = (proj_q, proj_k, proj_v)
    y, core, z, x = (lax.axis_index(name) for name in ALL)
    second = jnp.where(core == 0, x, z)

    received = [send(take_columns(half, grads), CORE_SWAP) for half in range(2)]
    transposed = order_projectors(projectors)

    def reduce_half(half):
        *pieces, own = project(half, transposed, grads, received[half])
        arrived = [send(piece.astype(F16), along_first(d)) for d, piece in zip(ORDER, pieces)]

        def regroup(parts, cut):
            total = cut(parts[0])
            for part in parts[1:]:
                total = total + cut(part)
            return total

        if half == 0:
            *parts, kept = combine(half, own, arrived)
            parts = [kept, *[send(part, along_y(d)) for d, part in zip(ORDER, parts)]]

            def last(b):
                return regroup(
                    parts, lambda x: lax.dynamic_slice_in_dim(x, b * RANK_ROWS, RANK_ROWS, axis=0)
                )

            blocks = {d: last((second + d) % 4) for d in ORDER}
            return [blocks[0], *[send(blocks[d], along_second(d)) for d in ORDER[:3]]]

        *parts, kept = combine(half, own, arrived)
        parts = [kept, *[send(part, along_second(d)) for d, part in zip(ORDER, parts)]]

        def last(b):
            return regroup(parts, lambda x: lax.dynamic_slice_in_dim(x, b * HALF, HALF, axis=1))

        blocks = {d: last((y + d) % 4) for d in ORDER}
        return [blocks[0], *[send(blocks[d], along_y(d)) for d in ORDER[:3]]]

    projected, square_sum = finish_sum([reduce_half(half) for half in range(2)])
    square_sum = square_sum + send(square_sum, CORE_SWAP)
    for along in (along_y, along_first, along_second):
        a, b, c = (send(square_sum, along(d)) for d in ORDER[:3])
        square_sum = (square_sum + a) + (b + c)

    *moments, update = adam(
        projected,
        square_sum,
        (avg_q, key_first_moment, value_first_moment),
        (sq_q, key_second_moment, value_second_moment),
    )

    near = {d: send(update, along_second(d)) for d in ORDER[:3]}
    held = jnp.concatenate([update, near[1], near[2], near[3]], axis=0)
    far = {d: send(held, along_first(d)) for d in ORDER[:3]}
    gathered = [held, far[1], far[2], far[3]]
    new_weights = apply_updates(
        gathered,
        projectors,
        (weight_q, key_weight_matrix, value_weight_matrix),
        (comp_q, key_compensation, value_compensation),
    )
    return (*new_weights, *moments)


def solution(mesh):
    split = Mesh(mesh.devices.reshape(4, 2, 4, 4), ALL)
    return jax.shard_map(
        shards,
        mesh=split,
        in_specs=(*[P(DP, FSDP, None)] * 3, *[P(FSDP, None)] * 3, *[P(FSDP, DP)] * 12),
        out_specs=(*[P(FSDP, DP)] * 9,),
        check_vma=False,
    )
```
